32 devices in a mesh: seq: 8 (over z, y), head: 4 (over x, core).
Axes of the slice: x: 2, y: 2, z: 4, core: 2. Of those that a mesh axis runs over, the one named last changes fastest.
Arguments:
- tokens: bfloat16 [6144, 2560], P(('seq', 'head')), may hold values from -12 to 12
- pre_gain: float32 [2560], replicated, may hold values from 0.25 to 1.75
- inner_proj: bfloat16 [2560, 2, 5120], P(None, None, 'head'), may hold values from -0.125 to 0.125
- outer_proj: bfloat16 [2560, 336], replicated, may hold values from -0.125 to 0.125
- kernel_x: float32 [4, 5120], P(None, 'head'), may hold values from -3 to 3
- kernel_bc: float32 [4, 256], replicated, may hold values from -3 to 3
- offset_x: float32 [5120], P('head'), may hold values from -3 to 3
- offset_bc: float32 [256], replicated, may hold values from -3 to 3
- dt_bias: float32 [80], P('head'), may hold values from -7 to -5
- a_log: float32 [80], P('head'), may hold values from -12 to 4
- skip_gain: float32 [80], P('head'), may hold values from 0.5 to 1.5
- norm_gain: float32 [5120], P('head'), may hold values from 0.25 to 1.75
- out_proj: bfloat16 [5120, 2560], P('head'), may hold values from -0.078125 to 0.078125
Outputs:
- mixed: bfloat16 [6144, 2560], P(('seq', 'head'))
The draws below stay inside these ranges and needn't reach their ends.
All inputs are finite; a program needn't handle non-finite values.
Results may differ from the reference program's by a relative error of at most 0.014.
Values may be sent and summed in bfloat16 or wider, within the bound.
A program may use at most 128 MiB of HBM per device.

```python
import jax
import jax.numpy as jnp
from jax import lax

D = 2560
H = 80
P_SIZE = 64
N = 128
CONV = 4
SPAN = 256
DI = 5120
TOKENS = 6144
N_HEAD = 4


def draw_tokens(key, part):
    noise_key, level_key, course_key = jax.random.split(key, 3)
    blocks = TOKENS // SPAN
    noise = jax.random.normal(noise_key, (TOKENS, D), jnp.float32)
    levels = 2.0 * jax.random.normal(level_key, (blocks, 1, 1), jnp.float32)
    course = jax.random.normal(course_key, (1, 1, D), jnp.float32)
    shifted = noise.reshape(blocks, SPAN, D) + levels * course
    return jnp.clip(shifted.reshape(TOKENS, D), -12.0, 12.0).astype(jnp.bfloat16)


def draw_a_log(key, part):
    order_key, rate_key = jax.random.split(key)
    order = jax.random.permutation(order_key, H)
    share = H // 2
    quick = order < share
    spread = jax.random.uniform(rate_key, (H,), jnp.float32)
    quick_rate = jnp.log(4.0) + spread * jnp.log(10.0)
    patient_rate = jnp.log(10.0 / TOKENS) + spread * jnp.log(10.0)
    return jnp.where(quick, quick_rate, patient_rate).astype(jnp.float32)


def block_levels(own_key, dims, cuts, least, top_value):
    level = 1.0
    for dim, blocks in cuts:
        heights = jax.random.uniform(jax.random.fold_in(jax.random.fold_in(own_key, 6), dim), (blocks,), jnp.float32, least / len(cuts), top_value / len(cuts))
        level = level * jnp.repeat(jnp.exp(heights), dims[dim] // blocks).reshape((-1,) + (1,) * (len(dims) - 1 - dim))
    return level


def normal_values(stream_key, dims, scale, limit, cuts=(), kind=jnp.bfloat16):
    drawn = jax.random.normal(stream_key, dims, jnp.float32) * scale
    if len(cuts) > 0:
        drawn = block_levels(stream_key, dims, cuts, -0.22, 0.18) * drawn
    return jnp.clip(drawn, min=-limit, max=limit).astype(kind)


def setup_inputs(seed: int = 0) -> dict:
    streams_of = jax.random.split(jax.random.key(seed), 14)
    tokens = draw_tokens(jax.random.fold_in(streams_of[13], 71), 0)
    pre_gain = jnp.clip(1.0 + 0.15 * jax.random.normal(streams_of[1], (D,), jnp.float32), 0.25, 1.75)
    inner_proj = normal_values(streams_of[2], (D, 2, DI), D ** -0.5, 0.125, ((2, 4),))
    outer_proj = normal_values(streams_of[3], (D, 2 * N + H), D ** -0.5, 0.125)
    kernel_x = normal_values(streams_of[4], (CONV, DI), CONV ** -0.5, 3.0, ((1, 4),), jnp.float32)
    kernel_bc = normal_values(streams_of[5], (CONV, 2 * N), CONV ** -0.5, 3.0, (), jnp.float32)
    offset_x = normal_values(streams_of[6], (DI,), 0.5, 3.0, ((0, 4),), jnp.float32)
    offset_bc = normal_values(streams_of[7], (2 * N,), 0.5, 3.0, (), jnp.float32)
    dt_bias = jnp.clip(-7.0 + 2.0 * jax.random.uniform(streams_of[8], (H,), jnp.float32) ** block_levels(streams_of[8], (H,), ((0, 4),), -0.2, 0.2), -7.0, -5.0)
    a_log = draw_a_log(jax.random.fold_in(streams_of[13], 71), 0)
    skip_gain = jnp.clip(0.5 + 1.0 * jax.random.uniform(streams_of[10], (H,), jnp.float32) ** block_levels(streams_of[10], (H,), ((0, 4),), -0.2, 0.2), 0.5, 1.5)
    norm_gain = jnp.clip(1.0 + 0.15 * jax.random.normal(streams_of[11], (DI,), jnp.float32), 0.25, 1.75)
    out_proj = normal_values(streams_of[12], (DI, D), DI ** -0.5, 0.078125, ((0, 4),))
    return {"tokens": tokens, "pre_gain": pre_gain, "inner_proj": inner_proj, "outer_proj": outer_proj, "kernel_x": kernel_x, "kernel_bc": kernel_bc, "offset_x": offset_x, "offset_bc": offset_bc, "dt_bias": dt_bias, "a_log": a_log, "skip_gain": skip_gain, "norm_gain": norm_gain, "out_proj": out_proj}


norm_floor = 0.1

def row_norm(row_block, gain_vector):
    widened = row_block.astype(jnp.float32)
    inverse_rms = lax.rsqrt(lax.optimization_barrier(jnp.mean(widened * widened, axis=-1, keepdims=True)) + norm_floor)
    return widened * inverse_rms * gain_vector

def masked_exp(log_gap, causal):
    return jnp.where(causal, jnp.exp(jnp.where(causal, log_gap, 0.0)), 0.0)

def block_scan(values_x, values_b, values_c, step_sizes, decay_rate, ssm_state):
    running = jnp.cumsum(step_sizes * decay_rate, axis=0)
    score_rows = jnp.dot(values_c, values_b.T, preferred_element_type=jnp.float32)
    running_heads = running.T
    row_index = lax.broadcasted_iota(jnp.int32, (SPAN, SPAN), 0)
    col_index = lax.broadcasted_iota(jnp.int32, (SPAN, SPAN), 1)
    decay_factor = masked_exp(running_heads[:, :, None] - running_heads[:, None, :], row_index >= col_index)
    mix_weights = (score_rows[None] * decay_factor * step_sizes.T[:, None, :]).astype(jnp.bfloat16)
    intra_out = jnp.einsum('hts,shp->thp', mix_weights.astype(jnp.float32), values_x.astype(jnp.float32))
    end_weight = jnp.exp(running[-1:] - running) * step_sizes
    scaled_x = (values_x.astype(jnp.float32) * end_weight[:, :, None]).astype(jnp.bfloat16)
    block_state = jnp.einsum('shp,sn->hpn', scaled_x.astype(jnp.float32), values_b.astype(jnp.float32))
    cross_out = jnp.exp(running)[:, :, None] * jnp.einsum('tn,hpn->thp', values_c.astype(jnp.float32), ssm_state, precision=lax.Precision.HIGHEST)
    next_state = jnp.exp(running[-1])[:, None, None] * ssm_state + block_state
    return (intra_out + cross_out, next_state)

def reference(tokens, pre_gain, inner_proj, outer_proj, kernel_x, kernel_bc, offset_x, offset_bc, dt_bias, a_log, skip_gain, norm_gain, out_proj):
    decay_rate = -jnp.exp(a_log)
    joined_proj = inner_proj.reshape(D, 2 * DI)
    conv_weight = jnp.concatenate([kernel_x, kernel_bc], axis=1)
    conv_bias = jnp.concatenate([offset_x, offset_bc])
    group_width = DI // N_HEAD

    def advance(carry, row_block):
        ssm_state, conv_tail = carry
        normed = row_norm(row_block, pre_gain).astype(jnp.bfloat16)
        inner_part = jnp.dot(normed, joined_proj, preferred_element_type=jnp.float32)
        outer_part = jnp.dot(normed, outer_proj, preferred_element_type=jnp.float32)
        gate_in = inner_part[:, :DI].astype(jnp.bfloat16)
        x_in = inner_part[:, DI:].astype(jnp.bfloat16)
        bc_in = outer_part[:, :2 * N].astype(jnp.bfloat16)
        dt_raw = outer_part[:, 2 * N:]
        conv_input = jnp.concatenate([x_in, bc_in], axis=1)
        extended = jnp.concatenate([conv_tail, conv_input], axis=0)
        summed = jnp.broadcast_to(conv_bias, conv_input.shape).astype(jnp.float32)
        for offset in range(CONV):
            summed = summed + conv_weight[offset] * extended[offset:offset + SPAN].astype(jnp.float32)
        conv_out = jax.nn.silu(summed).astype(jnp.bfloat16)
        values_x = conv_out[:, :DI].reshape(SPAN, H, P_SIZE)
        values_b = conv_out[:, DI:DI + N]
        values_c = conv_out[:, DI + N:]
        step_sizes = jax.nn.softplus(dt_raw + dt_bias)
        scan_out, next_state = block_scan(values_x, values_b, values_c, step_sizes, decay_rate, ssm_state)
        mixer_out = (scan_out + skip_gain[:, None] * values_x.astype(jnp.float32)).reshape(SPAN, DI)
        gated = mixer_out * jax.nn.silu(gate_in.astype(jnp.float32))
        normed_out = row_norm(gated, norm_gain).astype(jnp.bfloat16)
        total = jnp.zeros((SPAN, D), jnp.float32)
        for offset in range(N_HEAD):
            lower = offset * group_width
            partial_value = jnp.dot(normed_out[:, lower:lower + group_width], out_proj[lower:lower + group_width], preferred_element_type=jnp.float32).astype(jnp.bfloat16)
            total = total + lax.optimization_barrier(partial_value).astype(jnp.float32)
        next_tail = extended[SPAN:]
        return ((next_state, next_tail), total.astype(jnp.bfloat16))
    start_state = jnp.zeros((H, P_SIZE, N), jnp.float32)
    start_tail = jnp.zeros((CONV - 1, DI + 2 * N), jnp.bfloat16)
    blocks_in = tokens.reshape(TOKENS // SPAN, SPAN, D)
    final_carry, outputs = lax.scan(advance, (start_state, start_tail), blocks_in)
    return outputs.reshape(TOKENS, D)
```

```python
import functools

import jax
import jax.numpy as jnp
from jax import lax
from jax.experimental import pallas as pl
from jax.experimental.pallas import tpu as pltpu
from jax.sharding import PartitionSpec as P

SPAN = 256
HALO = 8
LANES = 128
PIECE = 512
CORES = 2
FEED = 512
DEPTH = 256

norm_floor = 0.1


def silu(value):
    half = 0.5 * value
    return half * jnp.tanh(half) + half


def softplus(value):
    small = jnp.exp(-jnp.abs(value))
    series = small * (1.0 - small * (0.5 - small * (1.0 / 3.0 - small * 0.25)))
    return jnp.maximum(value, 0.0) + jnp.where(small < 0.03, series, jnp.log(1.0 + small))


def in_two(value):
    top = value.astype(jnp.bfloat16)
    return top, (value - top.astype(jnp.float32)).astype(jnp.bfloat16)


def in_three(value):
    top = value.astype(jnp.bfloat16)
    rest = value - top.astype(jnp.float32)
    middle = rest.astype(jnp.bfloat16)
    return top, middle, (rest - middle.astype(jnp.float32)).astype(jnp.bfloat16)


def layer_kernel(
    sizes,
    tokens_hbm,
    pre_gain_ref,
    inner_hbm,
    outer_hbm,
    kernel_x_ref,
    kernel_bc_ref,
    offset_x_ref,
    offset_bc_ref,
    dt_bias_ref,
    a_log_ref,
    skip_gain_ref,
    norm_gain_ref,
    proj_hbm,
    out_ref,
    tok,
    tok_in,
    raw,
    gate_w,
    inner_w,
    outer_w,
    proj,
    gate,
    ext_x,
    ext_bc,
    dt_buf,
    halo_x,
    halo_bc,
    halo_x_out,
    halo_bc_out,
    conv_x,
    conv_bc,
    y_buf,
    cum_buf,
    states,
    carried,
    sum_out,
    sum_in,
    rate_out,
    rate_in,
    carry_out,
    carry_in,
    normed,
    sq_out,
    sq_in,
    inv_col,
    pair_out,
    pair_in,
    chip_out,
    chip_in,
    keep,
    small,
    tok_sem,
    raw_sems,
    load_sems,
    row_send,
    row_recv,
    mate_send,
    mate_recv,
    halo_sems,
    sum_send,
    sum_recv,
    rate_send,
    rate_recv,
    carry_send,
    carry_recv,
    sq_send,
    sq_recv,
    pair_send,
    pair_recv,
    chip_send,
    chip_recv,
):
    devices, groups, rows, model, width, state, taps, head_count = sizes
    f32, bf16 = jnp.float32, jnp.bfloat16
    head_size = width // head_count
    blocks = rows // SPAN
    share = state // devices
    total_width = width * groups
    own_rows = rows // groups
    chips = groups // CORES
    chip_rows = own_rows * CORES
    feeds = model // FEED
    steps = model // DEPTH
    strips = width // LANES
    me = lax.axis_index("seq")
    group = lax.axis_index("head")
    chip, core = group // CORES, lax.rem(group, CORES)
    partner = group + 1 - 2 * core
    seq_peer = [lax.rem(me + o, devices) for o in range(devices)]
    seq_back = [lax.rem(me - o + devices, devices) for o in range(devices)]
    head_peer = [lax.rem(group + o, groups) for o in range(groups)]

    def remote(src, dst, send, recv, axis, peer):
        return pltpu.make_async_remote_copy(
            src_ref=src, dst_ref=dst, send_sem=send, recv_sem=recv, device_id={axis: peer}
        )

    own = pl.ds(pl.multiple_of(group * own_rows, 16), own_rows)
    load_tok = pltpu.make_async_copy(tokens_hbm, tok_in, tok_sem)
    load_tok.start()

    def raw_copy(step, slot, strip):
        return pltpu.make_async_copy(
            inner_hbm.at[pl.ds(pl.multiple_of(step * DEPTH, DEPTH), DEPTH), :, pl.ds(strip * LANES, LANES)],
            raw.at[slot, strip],
            raw_sems.at[slot, strip],
        )

    for strip in range(strips):
        raw_copy(0, 0, strip).start()
    load_outer = pltpu.make_async_copy(outer_hbm, outer_w, load_sems.at[0])
    load_outer.start()
    for strip in range(strips):
        raw_copy(1, 1, strip).start()
    load_proj = pltpu.make_async_copy(proj_hbm, proj, load_sems.at[1])

    barrier = pltpu.get_barrier_semaphore()
    for o in range(1, devices):
        pl.semaphore_signal(barrier, 1, device_id={"seq": seq_peer[o]})
    for o in range(1, groups):
        pl.semaphore_signal(barrier, 1, device_id={"head": head_peer[o]})

    small[...] = jnp.zeros_like(small)
    small[0:1, 0:head_count] = dt_bias_ref[...].reshape(1, head_count)
    small[1:2, 0:head_count] = -jnp.exp(a_log_ref[...].reshape(1, head_count))
    small[2:3, 0:head_count] = skip_gain_ref[...].reshape(1, head_count)

    def clear(k, carry):
        row = pl.multiple_of(k * 64, 64)
        gate[pl.ds(row, 64), :] = jnp.zeros((64, width), f32)
        ext_x[pl.ds(8 + row, 64), :] = jnp.zeros((64, width), f32)
        ext_bc[pl.ds(8 + row, 64), :] = jnp.zeros((64, 2 * state), f32)
        dt_buf[pl.ds(row, 64), :] = jnp.zeros((64, LANES), f32)
        return carry

    def normalise(k, carry):
        row = pl.multiple_of(k * 16, 16)
        squares = jnp.zeros((16, LANES), f32)
        for column in range(0, model, LANES):
            value = tok_in[pl.ds(row, 16), pl.ds(column, LANES)].astype(f32)
            squares = squares + value * value
        inverse = lax.rsqrt(jnp.sum(squares, axis=1, keepdims=True) / model + norm_floor)
        for column in range(0, model, LANES):
            lanes = pl.ds(column, LANES)
            value = tok_in[pl.ds(row, 16), lanes].astype(f32)
            tok[pl.ds(pl.multiple_of(group * own_rows + row, 16), 16), lanes] = (
                value * inverse * pre_gain_ref[lanes].reshape(1, LANES)
            ).astype(bf16)
        return carry

    load_tok.wait()
    lax.fori_loop(0, own_rows // 16, normalise, 0)
    pl.semaphore_wait(barrier, devices + groups - 2)

    def feed_at(chip_index, core_index, feed):
        begin = pl.multiple_of((chip_index * CORES + core_index) * own_rows, 16)
        return tok.at[pl.ds(begin, own_rows), pl.ds(pl.multiple_of(feed * FEED, FEED), FEED)]

    def mate_copy(o, feed):
        piece = feed_at(lax.rem(chip - o + chips, chips), core, feed)
        return remote(piece, piece, mate_send.at[o, feed], mate_recv.at[o, feed], "head", partner)

    def row_copy(o, feed):
        piece = feed_at(chip, core, feed)
        target = lax.rem(chip + o, chips) * CORES + core
        return remote(piece, piece, row_send.at[o, feed], row_recv.at[o, feed], "head", target)

    for feed in range(feeds):
        for o in range(1, chips):
            row_copy(o, feed).start()
    for feed in range(feeds):
        mate_copy(0, feed).start()
    lax.fori_loop(0, rows // 64, clear, 0)

    out_row = lax.broadcasted_iota(jnp.int32, (DEPTH, DEPTH), 0)
    in_row = lax.broadcasted_iota(jnp.int32, (DEPTH, DEPTH), 1)
    half_depth = DEPTH // 2
    parting = (
        in_row == jnp.where(out_row < half_depth, 2 * out_row, 2 * (out_row - half_depth) + 1)
    ).astype(f32).astype(bf16)

    def separate(step, slot):
        for lower in range(0, strips, 2):
            members = range(lower, min(lower + 2, strips))
            columns = pl.ds(lower * LANES, len(members) * LANES)
            for part in range(2):
                parts = [
                    raw.at[slot, m].reshape(2 * DEPTH, LANES)[pl.ds(part * DEPTH, DEPTH), :]
                    for m in members
                ]
                both = jnp.dot(
                    parting, jnp.concatenate(parts, axis=1), preferred_element_type=f32
                ).astype(bf16)
                begin = pl.multiple_of(step * DEPTH + part * half_depth, half_depth)
                gate_w[pl.ds(begin, half_depth), columns] = both[:half_depth]
                inner_w[pl.ds(begin, half_depth), columns] = both[half_depth:]

    tile = 256 if width % 256 == 0 else LANES

    def rows_of(base, begin, depth):
        return tok[pl.ds(pl.multiple_of(base, 16), chip_rows), pl.ds(begin, depth)]

    def gather_into(target, offset, base, weight, begin, depth):
        here = pl.ds(pl.multiple_of(base + offset, 8), chip_rows)
        for column in range(0, width, tile):
            columns = pl.ds(column, tile)
            target[here, columns] += jnp.dot(
                rows_of(base, begin, depth), weight[pl.ds(begin, depth), columns],
                preferred_element_type=f32,
            )

    def gather_outer(base, begin, depth):
        result = lax.dot_general(
            rows_of(base, begin, depth), outer_w[:, pl.ds(begin, depth)], (((1,), (1,)), ((), ())),
            preferred_element_type=f32,
        )
        ext_bc[pl.ds(pl.multiple_of(base + 8, 8), chip_rows), :] += result[:, : 2 * state]
        raw_columns = result.shape[1] - 2 * state
        dt_buf[pl.ds(pl.multiple_of(base, 8), chip_rows), pl.ds(0, raw_columns)] += result[:, 2 * state :]

    local_base = pl.multiple_of(chip * chip_rows, 32)
    load_outer.wait()

    def local_step(step, carry):
        slot = lax.rem(step, 2)
        for strip in range(strips):
            raw_copy(step, slot, strip).wait()
        separate(step, slot)

        @pl.when(step + 2 < steps)
        def _():
            for strip in range(strips):
                raw_copy(step + 2, slot, strip).start()

        @pl.when(lax.rem(step, FEED // DEPTH) == 0)
        def _():
            mate_copy(0, step // (FEED // DEPTH)).wait_recv()

        begin = pl.multiple_of(step * DEPTH, DEPTH)
        gather_into(ext_x, 8, local_base, inner_w, begin, DEPTH)
        gather_outer(local_base, begin, DEPTH)
        gather_into(gate, 0, local_base, gate_w, begin, DEPTH)
        return carry

    lax.fori_loop(0, steps, local_step, 0)
    load_proj.start()

    bias_row, rate_row = small[0:1, :], small[1:2, :]
    own_lane = lax.broadcasted_iota(jnp.int32, (32, LANES), 1) < head_count

    def finish_rows(base):
        def step(k, carry):
            row = pl.multiple_of(base + k * 32, 32)
            here, lower = pl.ds(row, 32), pl.ds(row + 8, 32)
            for target, columns in ((ext_x, width), (ext_bc, 2 * state)):
                for column in range(0, columns, LANES):
                    lanes = pl.ds(column, LANES)
                    target[lower, lanes] = target[lower, lanes].astype(bf16).astype(f32)
            raw_steps = pltpu.roll(dt_buf[here, :], lax.rem(LANES - group * head_count, LANES), 1)
            dt_buf[here, :] = jnp.where(own_lane, softplus(raw_steps + bias_row), 0.0)
            return carry

        lax.fori_loop(0, chip_rows // 32, step, 0)

    def finish_gate(base):
        def step(k, carry):
            here = pl.ds(pl.multiple_of(base + k * 32, 32), 32)
            for column in range(0, width, LANES):
                lanes = pl.ds(column, LANES)
                gate[here, lanes] = silu(gate[here, lanes].astype(bf16).astype(f32))
            return carry

        lax.fori_loop(0, chip_rows // 32, step, 0)

    def convolve(source, weight, bias, target, columns, row):
        for lower in range(0, columns, LANES):
            lanes = pl.ds(lower, LANES)
            window = source[pl.ds(row, 40), lanes]
            total = jnp.broadcast_to(bias[lanes].reshape(1, LANES), (32, LANES))
            for tap in range(taps):
                shift = 8 - taps + 1 + tap
                total = total + weight[tap : tap + 1, lanes] * window[shift : shift + 32]
            target[pl.ds(row, 32), lanes] = silu(total).astype(bf16)

    def convolve_rows(begin, first, last):
        def step(k, carry):
            row = pl.multiple_of(begin + k * 32, 32)
            convolve(ext_bc, kernel_bc_ref, offset_bc_ref, conv_bc, 2 * state, row)
            convolve(ext_x, kernel_x_ref, offset_x_ref, conv_x, width, row)
            return carry

        lax.fori_loop(first, last, step, 0)

    finish_rows(local_base)
    convolve_rows(local_base, 1, chip_rows // 32)

    def far_base(o):
        return pl.multiple_of(lax.rem(chip - o + chips, chips) * chip_rows, 32)

    def take_feed(o, feed):
        row_copy(o, feed).wait_recv()
        mate_copy(o, feed).start()

    def far_step(o, feed):
        mate_copy(o, feed).wait_recv()
        begin = pl.multiple_of(feed * FEED, FEED)
        gather_into(ext_x, 8, far_base(o), inner_w, begin, FEED)
        gather_outer(far_base(o), begin, FEED)

    def far_gate(o, feed):
        gather_into(gate, 0, far_base(o), gate_w, pl.multiple_of(feed * FEED, FEED), FEED)

    for o in range(1, chips):
        take_feed(o, 0)

        def far_loop(feed, carry):
            take_feed(o, feed + 1)
            far_step(o, feed)
            far_gate(o, feed)
            return carry

        lax.fori_loop(0, feeds - 1, far_loop, 0)
        far_step(o, feeds - 1)
        finish_rows(far_base(o))
        if o < chips - 1:
            far_gate(o, feeds - 1)

    halo_x_out[...] = ext_x[pl.ds(rows, HALO), :]
    halo_bc_out[...] = ext_bc[pl.ds(rows, HALO), :]
    halo_copies = [
        remote(halo_x_out, halo_x, halo_sems.at[0], halo_sems.at[1], "seq", seq_peer[1]),
        remote(halo_bc_out, halo_bc, halo_sems.at[2], halo_sems.at[3], "seq", seq_peer[1]),
    ]
    for copy in halo_copies:
        copy.start()
    for o in range(1, chips):
        convolve_rows(far_base(o), 1, chip_rows // 32)
    for block in range(1, chips):
        convolve_rows(block * chip_rows, 0, 1)

    head_of_lane = lax.broadcasted_iota(jnp.int32, (LANES, width), 1) // head_size
    spread = (
        (head_of_lane == lax.broadcasted_iota(jnp.int32, (LANES, width), 0)).astype(f32).astype(bf16)
    )
    spread_two = jnp.concatenate([spread, spread], axis=0)
    lower_tri = (
        lax.broadcasted_iota(jnp.int32, (SPAN, SPAN), 0)
        >= lax.broadcasted_iota(jnp.int32, (SPAN, SPAN), 1)
    ).astype(f32).astype(bf16)

    def spread_rows(value):
        return jnp.dot(
            jnp.concatenate(in_two(value), axis=1), spread_two, preferred_element_type=f32
        )

    def spread_exact(value):
        total = 0.0
        for part in in_three(value):
            total = total + jnp.dot(part, spread, preferred_element_type=f32)
        return total

    skip_wide = spread_exact(jnp.broadcast_to(small[2:3, :], (8, LANES)))[0:1]
    lasts = []
    for block in range(blocks):
        span = pl.ds(block * SPAN, SPAN)
        parts = jnp.dot(
            lower_tri, jnp.concatenate(in_three(dt_buf[span, :] * rate_row), axis=1),
            preferred_element_type=f32,
        )
        running = parts[:, :LANES] + parts[:, LANES : 2 * LANES] + parts[:, 2 * LANES :]
        cum_buf[span, :] = running
        lasts.append(running[SPAN - 1 : SPAN, :])

    for copy in halo_copies:
        copy.wait()
    first = me > 0
    ext_x[0:8, :] = jnp.where(first, halo_x[...], 0.0)
    ext_bc[0:8, :] = jnp.where(first, halo_bc[...], 0.0)
    convolve_rows(0, 0, 1)

    prefix = jnp.zeros((1, LANES), f32)
    prefixes = []
    for block in range(blocks):
        span = pl.ds(block * SPAN, SPAN)
        last = lasts[block]
        end_weight = spread_rows(jnp.exp(last - cum_buf[span, :]) * dt_buf[span, :])
        scaled = (conv_x[span, :].astype(f32) * end_weight).astype(bf16)
        new_state = lax.dot_general(
            conv_bc[span, pl.ds(0, state)], scaled, (((0,), (0,)), ((), ())),
            preferred_element_type=f32,
        )
        if block > 0:
            decay = spread_exact(jnp.broadcast_to(jnp.exp(last), (8, LANES)))[0:1]
            new_state = decay * states[block - 1] + new_state
        states[block] = new_state
        prefixes.append(prefix)
        prefix = prefix + last

    for j in range(devices):
        sum_out[j] = states[blocks - 1, pl.ds(j * share, share), :].astype(bf16)
    rate_out[...] = jnp.broadcast_to(prefix, (8, LANES))

    sum_copies, rate_copies = [], []
    for o in range(1, devices):
        sum_copies.append(
            remote(
                sum_out.at[seq_peer[o]], sum_in.at[o], sum_send.at[o], sum_recv.at[o],
                "seq", seq_peer[o],
            )
        )
        rate_copies.append(
            remote(
                rate_out, rate_in.at[o], rate_send.at[o], rate_recv.at[o], "seq", seq_peer[o]
            )
        )
    for a, b in zip(sum_copies, rate_copies):
        b.start()
        a.start()

    for o in range(max(chips - 1, 1), chips):
        far_gate(o, feeds - 1)

    row_index = lax.broadcasted_iota(jnp.int32, (LANES, LANES), 0)
    col_index = lax.broadcasted_iota(jnp.int32, (LANES, LANES), 1)
    causal = row_index >= col_index
    lane_index = lax.broadcasted_iota(jnp.int32, (SPAN, LANES), 1)
    pair = LANES // head_size

    def inside(block):
        span = pl.ds(pl.multiple_of(block * SPAN, SPAN), SPAN)
        running = cum_buf[span, :]
        running_t = running.T
        steps_t = dt_buf[span, :].T
        scores = lax.dot_general(
            conv_bc[span, pl.ds(state, state)], conv_bc[span, pl.ds(0, state)],
            (((1,), (1,)), ((), ())), preferred_element_type=f32,
        )
        half = SPAN // 2
        for strip in range(strips):
            lanes = pl.ds(strip * LANES, LANES)
            value = conv_x[span, lanes]
            upper, bottom, stacked_top, stacked = [], [], [], []
            for member in range(pair):
                head = strip * pair + member
                column = running[:, head : head + 1]
                line = running_t[head : head + 1, :]
                steps_line = steps_t[head : head + 1, :]

                def weights(r, c):
                    rs, cs = slice(r * half, (r + 1) * half), slice(c * half, (c + 1) * half)
                    gap = column[rs] - line[:, cs]
                    if r == c:
                        gap = jnp.where(causal, gap, -1e30)
                    return (scores[rs, cs] * jnp.exp(gap) * steps_line[:, cs]).astype(bf16)

                upper.append(weights(0, 0))
                bottom.extend([weights(1, 0), weights(1, 1)])
                mine = jnp.where(lane_index // head_size == member, value, jnp.zeros_like(value))
                stacked_top.append(mine[:half])
                stacked.append(mine)
            top_out = jnp.dot(
                jnp.concatenate(upper, axis=1), jnp.concatenate(stacked_top, axis=0),
                preferred_element_type=f32,
            )
            bottom_out = jnp.dot(
                jnp.concatenate(bottom, axis=1), jnp.concatenate(stacked, axis=0),
                preferred_element_type=f32,
            )
            both = jnp.concatenate([top_out, bottom_out], axis=0)
            y_buf[span, lanes] = both + skip_wide[:, strip * LANES : (strip + 1) * LANES] * value.astype(f32)

    early = max(blocks - 1, 1)

    def inside_step(block, carry):
        inside(block)
        return carry

    lax.fori_loop(0, early, inside_step, 0)

    for a, b in zip(sum_copies, rate_copies):
        b.wait()
        a.wait()
    sum_in[0] = sum_out[me]
    rate_in[0] = rate_out[...]

    running_state = jnp.zeros((share, width), f32)
    for i in range(devices):
        slot = lax.rem(me - i + devices, devices)
        carry_out[slot] = running_state.astype(bf16)
        decay = spread_exact(jnp.exp(rate_in[slot]))[0:1]
        running_state = decay * running_state + sum_in[slot].astype(f32)

    carry_copies = []
    for o in range(1, devices):
        carry_copies.append(
            remote(
                carry_out.at[o], carry_in.at[o], carry_send.at[o], carry_recv.at[o],
                "seq", seq_back[o],
            )
        )
    for copy in carry_copies:
        copy.start()
    lax.fori_loop(early, blocks, inside_step, 0)
    for o in range(chips):
        finish_gate(o * chip_rows)
    load_proj.wait()
    for copy in carry_copies:
        copy.wait()
    carry_in[0] = carry_out[0]
    for j in range(devices):
        slot = lax.rem(j - me + devices, devices)
        carried[pl.ds(j * share, share), :] = carry_in[slot].astype(f32)

    squares = []
    for block in range(blocks):
        span = pl.ds(block * SPAN, SPAN)
        entry_decay = spread_exact(jnp.broadcast_to(jnp.exp(prefixes[block]), (8, LANES)))[0:1]
        entering = entry_decay * carried[...]
        if block > 0:
            entering = entering + states[block - 1]
        entering = entering.astype(bf16)
        growth = jnp.concatenate(in_two(jnp.exp(cum_buf[span, :])), axis=1)
        partial_sum = jnp.zeros((SPAN, LANES), f32)
        for strip in range(strips):
            lanes = pl.ds(strip * LANES, LANES)
            column = slice(strip * LANES, (strip + 1) * LANES)
            cross = jnp.dot(
                conv_bc[span, pl.ds(state, state)], entering[:, column],
                preferred_element_type=f32,
            )
            scale = jnp.dot(growth, spread_two[:, column], preferred_element_type=f32)
            gated = (y_buf[span, lanes] + scale * cross) * gate[span, lanes]
            partial_sum = partial_sum + gated * gated
            normed[span, lanes] = (gated * norm_gain_ref[lanes].reshape(1, LANES)).astype(bf16)
        squares.append(jnp.sum(partial_sum.T, axis=0, keepdims=True))
    own_squares = jnp.concatenate(squares, axis=1)
    sq_out[...] = jnp.broadcast_to(own_squares, (8, rows))
    sq_copies = []
    for o in range(1, groups):
        sq_copies.append(
            remote(sq_out, sq_in.at[o], sq_send.at[o], sq_recv.at[o], "head", head_peer[o])
        )
    for copy in sq_copies:
        copy.start()

    pieces = proj.shape[1] // PIECE
    jobs = [(o, q) for o in list(range(1, chips)) + [0] for q in range(pieces)]

    def pair_copy(o, q):
        return remote(
            pair_out.at[o, q], pair_in.at[o, q], pair_send.at[o, q], pair_recv.at[o, q],
            "head", partner,
        )

    def chip_copy(o, q):
        target = lax.rem(chip + o, chips) * CORES + core
        return remote(
            chip_out.at[o - 1, q], chip_in.at[o - 1, q], chip_send.at[o, q], chip_recv.at[o, q],
            "head", target,
        )

    def product(o, q, whose):
        base = lax.rem(chip + o, chips) * CORES * own_rows
        here = pl.ds(pl.multiple_of(base + whose * own_rows, 16), own_rows)
        return jnp.dot(normed[here, :], proj[:, pl.ds(q * PIECE, PIECE)], preferred_element_type=f32)

    def start_job(o, q):
        pair_out[o, q] = product(o, q, 1 - core).astype(bf16)
        pair_copy(o, q).start()

    def finish_job(o, q):
        result = product(o, q, core)
        pair_copy(o, q).wait()
        result = result + pair_in[o, q].astype(f32)
        if o > 0:
            chip_out[o - 1, q] = result.astype(bf16)
            chip_copy(o, q).start()
        else:
            keep[q] = result

    for index, job in enumerate(jobs):
        start_job(*job)
        if index > 0:
            finish_job(*jobs[index - 1])
    finish_job(*jobs[-1])

    for copy in sq_copies:
        copy.wait()
    total = own_squares
    for o in range(1, groups):
        total = total + sq_in[o, 0:1, :]
    inverse = lax.rsqrt(total / total_width + norm_floor)
    for block in range(blocks):
        part = jnp.broadcast_to(inverse[:, block * SPAN : (block + 1) * SPAN], (LANES, SPAN)).T
        inv_col[pl.ds(block * SPAN, SPAN), :] = part
    own_inverse = inv_col[own, :]

    for q in range(pieces):
        result = keep[q]
        for o in range(1, chips):
            chip_copy(o, q).wait()
            result = result + chip_in[o - 1, q].astype(f32)
        for lower in range(0, PIECE, LANES):
            out_ref[:, pl.ds(q * PIECE + lower, LANES)] = (
                result[:, lower : lower + LANES] * own_inverse
            ).astype(bf16)

    for feed in range(feeds):
        mate_copy(0, feed).wait_send()
        for o in range(1, chips):
            row_copy(o, feed).wait_send()
            mate_copy(o, feed).wait_send()


def layer_call(*operands):
    tokens, _, inner_proj, outer_proj, kernel_x, kernel_bc, _, _, dt_bias, _, _, _, out_proj = operands
    devices, groups = lax.axis_size("seq"), lax.axis_size("head")
    own_rows, model = tokens.shape
    width, taps, state = kernel_x.shape[1], kernel_x.shape[0], kernel_bc.shape[1] // 2
    rows = own_rows * groups
    blocks, share = rows // SPAN, state // devices
    chips, strips, feeds = groups // CORES, width // LANES, model // FEED
    chip_rows = own_rows * CORES
    pieces = model // PIECE
    sizes = (devices, groups, rows, model, width, state, taps, dt_bias.shape[0])
    f32, bf16 = jnp.float32, jnp.bfloat16
    sem = pltpu.SemaphoreType.DMA
    vmem, hbm = pl.BlockSpec(memory_space=pltpu.VMEM), pl.BlockSpec(memory_space=pl.ANY)
    return pl.pallas_call(
        functools.partial(layer_kernel, sizes),
        out_shape=jax.ShapeDtypeStruct((own_rows, model), bf16),
        in_specs=[hbm, vmem, hbm, hbm] + [vmem] * 8 + [hbm],
        out_specs=vmem,
        scratch_shapes=[
            pltpu.VMEM((rows, model), bf16),
            pltpu.VMEM((own_rows, model), bf16),
            pltpu.VMEM((2, strips, DEPTH, 2, LANES), bf16),
            pltpu.VMEM((model, width), bf16),
            pltpu.VMEM((model, width), bf16),
            pltpu.VMEM(outer_proj.shape, bf16),
            pltpu.VMEM(out_proj.shape, bf16),
            pltpu.VMEM((rows, width), f32),
            pltpu.VMEM((rows + 8, width), f32),
            pltpu.VMEM((rows + 8, 2 * state), f32),
            pltpu.VMEM((rows, LANES), f32),
            pltpu.VMEM((HALO, width), f32),
            pltpu.VMEM((HALO, 2 * state), f32),
            pltpu.VMEM((HALO, width), f32),
            pltpu.VMEM((HALO, 2 * state), f32),
            pltpu.VMEM((rows, width), bf16),
            pltpu.VMEM((rows, 2 * state), bf16),
            pltpu.VMEM((rows, width), f32),
            pltpu.VMEM((rows, LANES), f32),
            pltpu.VMEM((blocks, state, width), f32),
            pltpu.VMEM((state, width), f32),
            pltpu.VMEM((devices, share, width), bf16),
            pltpu.VMEM((devices, share, width), bf16),
            pltpu.VMEM((8, LANES), f32),
            pltpu.VMEM((devices, 8, LANES), f32),
            pltpu.VMEM((devices, share, width), bf16),
            pltpu.VMEM((devices, share, width), bf16),
            pltpu.VMEM((rows, width), bf16),
            pltpu.VMEM((8, rows), f32),
            pltpu.VMEM((groups, 8, rows), f32),
            pltpu.VMEM((rows, LANES), f32),
            pltpu.VMEM((chips, pieces, own_rows, PIECE), bf16),
            pltpu.VMEM((chips, pieces, own_rows, PIECE), bf16),
            pltpu.VMEM((chips - 1, pieces, own_rows, PIECE), bf16),
            pltpu.VMEM((chips - 1, pieces, own_rows, PIECE), bf16),
            pltpu.VMEM((pieces, own_rows, PIECE), f32),
            pltpu.VMEM((8, LANES), f32),
            sem,
            sem((2, strips)),
            sem((2,)),
            sem((chips, feeds)),
            sem((chips, feeds)),
            sem((chips, feeds)),
            sem((chips, feeds)),
            sem((4,)),
            sem((devices,)),
            sem((devices,)),
            sem((devices,)),
            sem((devices,)),
            sem((devices,)),
            sem((devices,)),
            sem((groups,)),
            sem((groups,)),
            sem((chips, pieces)),
            sem((chips, pieces)),
            sem((chips, pieces)),
            sem((chips, pieces)),
        ],
        compiler_params=pltpu.CompilerParams(
            collective_id=0, has_side_effects=True, vmem_limit_bytes=67043328
        ),
    )(*operands)


def on_device(*args):
    operands = list(args)
    operands[3] = operands[3].T
    return layer_call(*operands)


def solution(mesh):
    return jax.shard_map(
        on_device,
        mesh=mesh,
        in_specs=(
            P(("seq", "head"), None),
            P(),
            P(None, None, "head"),
            P(),
            P(None, "head"),
            P(),
            P("head"),
            P(),
            P("head"),
            P("head"),
            P("head"),
            P("head"),
            P("head", None),
        ),
        out_specs=P(("seq", "head"), None),
        check_vma=False,
    )
```

```python
import functools

import jax
import jax.numpy as jnp
from jax import lax
from jax.experimental import pallas as pl
from jax.experimental.pallas import tpu as pltpu
from jax.sharding import PartitionSpec as P

SPAN = 256
HALO = 8
LANES = 128
PIECE = 512
CORES = 2
FEED = 512
DEPTH = 256

norm_floor = 0.1


def silu(value):
    half = 0.5 * value
    return half * jnp.tanh(half) + half


def softplus(value):
    small = jnp.exp(-jnp.abs(value))
    series = small * (1.0 - small * (0.5 - small * (1.0 / 3.0 - small * 0.25)))
    return jnp.maximum(value, 0.0) + jnp.where(small < 0.03, series, jnp.log(1.0 + small))


def in_two(value):
    top = value.astype(jnp.bfloat16)
    return top, (value - top.astype(jnp.float32)).astype(jnp.bfloat16)


def in_three(value):
    top = value.astype(jnp.bfloat16)
    rest = value - top.astype(jnp.float32)
    middle = rest.astype(jnp.bfloat16)
    return top, middle, (rest - middle.astype(jnp.float32)).astype(jnp.bfloat16)


def layer_kernel(
    sizes,
    tokens_hbm,
    pre_gain_ref,
    inner_hbm,
    outer_hbm,
    kernel_x_ref,
    kernel_bc_ref,
    offset_x_ref,
    offset_bc_ref,
    dt_bias_ref,
    a_log_ref,
    skip_gain_ref,
    norm_gain_ref,
    proj_hbm,
    out_ref,
    tok,
    tok_in,
    raw,
    gate_w,
    inner_w,
    outer_w,
    proj,
    gate,
    ext_x,
    ext_bc,
    dt_buf,
    halo_x,
    halo_bc,
    halo_x_out,
    halo_bc_out,
    conv_x,
    conv_bc,
    y_buf,
    cum_buf,
    states,
    carried,
    sum_out,
    sum_in,
    rate_out,
    rate_in,
    carry_out,
    carry_in,
    normed,
    sq_out,
    sq_in,
    inv_col,
    entered,
    pair_out,
    pair_in,
    chip_out,
    chip_in,
    keep,
    small,
    tok_sem,
    raw_sems,
    load_sems,
    row_send,
    row_recv,
    mate_send,
    mate_recv,
    halo_sems,
    sum_send,
    sum_recv,
    rate_send,
    rate_recv,
    carry_send,
    carry_recv,
    sq_send,
    sq_recv,
    pair_send,
    pair_recv,
    chip_send,
    chip_recv,
):
    devices, groups, rows, model, width, state, taps, head_count = sizes
    f32, bf16 = jnp.float32, jnp.bfloat16
    head_size = width // head_count
    blocks = rows // SPAN
    share = state // devices
    total_width = width * groups
    own_rows = rows // groups
    chips = groups // CORES
    chip_rows = own_rows * CORES
    feeds = model // FEED
    steps = model // DEPTH
    strips = width // LANES
    me = lax.axis_index("seq")
    group = lax.axis_index("head")
    chip, core = group // CORES, lax.rem(group, CORES)
    partner = group + 1 - 2 * core
    seq_peer = [lax.rem(me + o, devices) for o in range(devices)]
    seq_back = [lax.rem(me - o + devices, devices) for o in range(devices)]
    head_peer = [lax.rem(group + o, groups) for o in range(groups)]

    def remote(src, dst, send, recv, axis, peer):
        return pltpu.make_async_remote_copy(
            src_ref=src, dst_ref=dst, send_sem=send, recv_sem=recv, device_id={axis: peer}
        )

    own = pl.ds(pl.multiple_of(group * own_rows, 16), own_rows)
    load_tok = pltpu.make_async_copy(tokens_hbm, tok_in, tok_sem)
    load_tok.start()

    def raw_copy(step, slot, strip):
        return pltpu.make_async_copy(
            inner_hbm.at[pl.ds(pl.multiple_of(step * DEPTH, DEPTH), DEPTH), :, pl.ds(strip * LANES, LANES)],
            raw.at[slot, strip],
            raw_sems.at[slot, strip],
        )

    for strip in range(strips):
        raw_copy(0, 0, strip).start()
    load_outer = pltpu.make_async_copy(outer_hbm, outer_w, load_sems.at[0])
    load_outer.start()
    for strip in range(strips):
        raw_copy(1, 1, strip).start()
    load_proj = pltpu.make_async_copy(proj_hbm, proj, load_sems.at[1])

    barrier = pltpu.get_barrier_semaphore()
    for o in range(1, devices):
        pl.semaphore_signal(barrier, 1, device_id={"seq": seq_peer[o]})
    for o in range(1, groups):
        pl.semaphore_signal(barrier, 1, device_id={"head": head_peer[o]})

    small[...] = jnp.zeros_like(small)
    small[0:1, 0:head_count] = dt_bias_ref[...].reshape(1, head_count)
    small[1:2, 0:head_count] = -jnp.exp(a_log_ref[...].reshape(1, head_count))
    small[2:3, 0:head_count] = skip_gain_ref[...].reshape(1, head_count)

    def clear(k, carry):
        row = pl.multiple_of(k * 64, 64)
        ext_x[pl.ds(8 + row, 64), :] = jnp.zeros((64, width), f32)
        ext_bc[pl.ds(8 + row, 64), :] = jnp.zeros((64, 2 * state), f32)
        dt_buf[pl.ds(row, 64), :] = jnp.zeros((64, LANES), f32)
        return carry

    def normalise(k, carry):
        row = pl.multiple_of(k * 16, 16)
        squares = jnp.zeros((16, LANES), f32)
        for column in range(0, model, LANES):
            value = tok_in[pl.ds(row, 16), pl.ds(column, LANES)].astype(f32)
            squares = squares + value * value
        inverse = lax.rsqrt(jnp.sum(squares, axis=1, keepdims=True) / model + norm_floor)
        for column in range(0, model, LANES):
            lanes = pl.ds(column, LANES)
            value = tok_in[pl.ds(row, 16), lanes].astype(f32)
            tok[pl.ds(pl.multiple_of(group * own_rows + row, 16), 16), lanes] = (
                value * inverse * pre_gain_ref[lanes].reshape(1, LANES)
            ).astype(bf16)
        return carry

    load_tok.wait()
    lax.fori_loop(0, own_rows // 16, normalise, 0)
    pl.semaphore_wait(barrier, devices + groups - 2)

    def feed_at(chip_index, core_index, feed):
        begin = pl.multiple_of((chip_index * CORES + core_index) * own_rows, 16)
        return tok.at[pl.ds(begin, own_rows), pl.ds(pl.multiple_of(feed * FEED, FEED), FEED)]

    def mate_copy(o, feed):
        piece = feed_at(lax.rem(chip - o + chips, chips), core, feed)
        return remote(piece, piece, mate_send.at[o, feed], mate_recv.at[o, feed], "head", partner)

    def row_copy(o, feed):
        piece = feed_at(chip, core, feed)
        target = lax.rem(chip + o, chips) * CORES + core
        return remote(piece, piece, row_send.at[o, feed], row_recv.at[o, feed], "head", target)

    for feed in range(feeds):
        for o in range(1, chips):
            row_copy(o, feed).start()
    for feed in range(feeds):
        mate_copy(0, feed).start()
    lax.fori_loop(0, rows // 64, clear, 0)

    out_row = lax.broadcasted_iota(jnp.int32, (DEPTH, DEPTH), 0)
    in_row = lax.broadcasted_iota(jnp.int32, (DEPTH, DEPTH), 1)
    half_depth = DEPTH // 2
    parting = (
        in_row == jnp.where(out_row < half_depth, 2 * out_row, 2 * (out_row - half_depth) + 1)
    ).astype(f32).astype(bf16)

    def separate(step, slot):
        for lower in range(0, strips, 2):
            members = range(lower, min(lower + 2, strips))
            columns = pl.ds(lower * LANES, len(members) * LANES)
            for part in range(2):
                parts = [
                    raw.at[slot, m].reshape(2 * DEPTH, LANES)[pl.ds(part * DEPTH, DEPTH), :]
                    for m in members
                ]
                both = jnp.dot(
                    parting, jnp.concatenate(parts, axis=1), preferred_element_type=f32
                ).astype(bf16)
                begin = pl.multiple_of(step * DEPTH + part * half_depth, half_depth)
                gate_w[pl.ds(begin, half_depth), columns] = both[:half_depth]
                inner_w[pl.ds(begin, half_depth), columns] = both[half_depth:]

    tile = 256 if width % 256 == 0 else LANES

    def rows_of(base, begin, depth):
        return tok[pl.ds(pl.multiple_of(base, 16), chip_rows), pl.ds(begin, depth)]

    def gather_into(target, offset, base, weight, begin, depth):
        here = pl.ds(pl.multiple_of(base + offset, 8), chip_rows)
        for column in range(0, width, tile):
            columns = pl.ds(column, tile)
            target[here, columns] += jnp.dot(
                rows_of(base, begin, depth), weight[pl.ds(begin, depth), columns],
                preferred_element_type=f32,
            )

    def gather_outer(base, begin, depth):
        result = lax.dot_general(
            rows_of(base, begin, depth), outer_w[:, pl.ds(begin, depth)], (((1,), (1,)), ((), ())),
            preferred_element_type=f32,
        )
        ext_bc[pl.ds(pl.multiple_of(base + 8, 8), chip_rows), :] += result[:, : 2 * state]
        raw_columns = result.shape[1] - 2 * state
        dt_buf[pl.ds(pl.multiple_of(base, 8), chip_rows), pl.ds(0, raw_columns)] += result[:, 2 * state :]

    local_base = pl.multiple_of(chip * chip_rows, 32)
    load_outer.wait()

    def local_step(step, carry):
        slot = lax.rem(step, 2)
        for strip in range(strips):
            raw_copy(step, slot, strip).wait()
        separate(step, slot)

        @pl.when(step + 2 < steps)
        def _():
            for strip in range(strips):
                raw_copy(step + 2, slot, strip).start()

        @pl.when(lax.rem(step, FEED // DEPTH) == 0)
        def _():
            mate_copy(0, step // (FEED // DEPTH)).wait_recv()

        begin = pl.multiple_of(step * DEPTH, DEPTH)
        gather_into(ext_x, 8, local_base, inner_w, begin, DEPTH)
        gather_outer(local_base, begin, DEPTH)
        return carry

    lax.fori_loop(0, steps, local_step, 0)
    load_proj.start()

    bias_row, rate_row = small[0:1, :], small[1:2, :]
    own_lane = lax.broadcasted_iota(jnp.int32, (32, LANES), 1) < head_count

    def finish_rows(base):
        def step(k, carry):
            row = pl.multiple_of(base + k * 32, 32)
            here, lower = pl.ds(row, 32), pl.ds(row + 8, 32)
            for target, columns in ((ext_x, width), (ext_bc, 2 * state)):
                for column in range(0, columns, LANES):
                    lanes = pl.ds(column, LANES)
                    target[lower, lanes] = target[lower, lanes].astype(bf16).astype(f32)
            raw_steps = pltpu.roll(dt_buf[here, :], lax.rem(LANES - group * head_count, LANES), 1)
            dt_buf[here, :] = jnp.where(own_lane, softplus(raw_steps + bias_row), 0.0)
            return carry

        lax.fori_loop(0, chip_rows // 32, step, 0)

    def fill_gate(base, size):
        here = pl.ds(pl.multiple_of(base, 16), size)
        for column in range(0, width, tile):
            columns = pl.ds(column, tile)
            gate_in = jnp.dot(tok[here, :], gate_w[:, columns], preferred_element_type=f32)
            gate[here, columns] = silu(gate_in.astype(bf16).astype(f32))

    def convolve(source, weight, bias, target, columns, row):
        for lower in range(0, columns, LANES):
            lanes = pl.ds(lower, LANES)
            window = source[pl.ds(row, 40), lanes]
            total = jnp.broadcast_to(bias[lanes].reshape(1, LANES), (32, LANES))
            for tap in range(taps):
                shift = 8 - taps + 1 + tap
                total = total + weight[tap : tap + 1, lanes] * window[shift : shift + 32]
            target[pl.ds(row, 32), lanes] = silu(total).astype(bf16)

    def convolve_rows(begin, first, last):
        def step(k, carry):
            row = pl.multiple_of(begin + k * 32, 32)
            convolve(ext_bc, kernel_bc_ref, offset_bc_ref, conv_bc, 2 * state, row)
            convolve(ext_x, kernel_x_ref, offset_x_ref, conv_x, width, row)
            return carry

        lax.fori_loop(first, last, step, 0)

    finish_rows(local_base)
    convolve_rows(local_base, 1, chip_rows // 32)

    def far_base(o):
        return pl.multiple_of(lax.rem(chip - o + chips, chips) * chip_rows, 32)

    def take_feed(o, feed):
        row_copy(o, feed).wait_recv()
        mate_copy(o, feed).start()

    def far_step(o, feed):
        mate_copy(o, feed).wait_recv()
        begin = pl.multiple_of(feed * FEED, FEED)
        gather_into(ext_x, 8, far_base(o), inner_w, begin, FEED)
        gather_outer(far_base(o), begin, FEED)

    for o in range(1, chips):
        take_feed(o, 0)

        def far_loop(feed, carry):
            take_feed(o, feed + 1)
            far_step(o, feed)
            return carry

        lax.fori_loop(0, feeds - 1, far_loop, 0)
        far_step(o, feeds - 1)
        finish_rows(far_base(o))

    halo_x_out[...] = ext_x[pl.ds(rows, HALO), :]
    halo_bc_out[...] = ext_bc[pl.ds(rows, HALO), :]
    halo_copies = [
        remote(halo_x_out, halo_x, halo_sems.at[0], halo_sems.at[1], "seq", seq_peer[1]),
        remote(halo_bc_out, halo_bc, halo_sems.at[2], halo_sems.at[3], "seq", seq_peer[1]),
    ]
    for copy in halo_copies:
        copy.start()
    for o in range(1, chips):
        convolve_rows(far_base(o), 1, chip_rows // 32)
    for block in range(1, chips):
        convolve_rows(block * chip_rows, 0, 1)

    head_of_lane = lax.broadcasted_iota(jnp.int32, (LANES, width), 1) // head_size
    spread = (
        (head_of_lane == lax.broadcasted_iota(jnp.int32, (LANES, width), 0)).astype(f32).astype(bf16)
    )
    spread_two = jnp.concatenate([spread, spread], axis=0)
    lower_tri = (
        lax.broadcasted_iota(jnp.int32, (SPAN, SPAN), 0)
        >= lax.broadcasted_iota(jnp.int32, (SPAN, SPAN), 1)
    ).astype(f32).astype(bf16)

    def spread_rows(value):
        return jnp.dot(
            jnp.concatenate(in_two(value), axis=1), spread_two, preferred_element_type=f32
        )

    def spread_exact(value):
        total = 0.0
        for part in in_three(value):
            total = total + jnp.dot(part, spread, preferred_element_type=f32)
        return total

    skip_wide = spread_exact(jnp.broadcast_to(small[2:3, :], (8, LANES)))[0:1]
    lasts = []
    for block in range(blocks):
        span = pl.ds(block * SPAN, SPAN)
        parts = jnp.dot(
            lower_tri, jnp.concatenate(in_three(dt_buf[span, :] * rate_row), axis=1),
            preferred_element_type=f32,
        )
        running = parts[:, :LANES] + parts[:, LANES : 2 * LANES] + parts[:, 2 * LANES :]
        cum_buf[span, :] = running
        lasts.append(running[SPAN - 1 : SPAN, :])

    for copy in halo_copies:
        copy.wait()
    first = me > 0
    ext_x[0:8, :] = jnp.where(first, halo_x[...], 0.0)
    ext_bc[0:8, :] = jnp.where(first, halo_bc[...], 0.0)
    convolve_rows(0, 0, 1)

    prefix = jnp.zeros((1, LANES), f32)
    prefixes = []
    for block in range(blocks):
        span = pl.ds(block * SPAN, SPAN)
        last = lasts[block]
        end_weight = spread_rows(jnp.exp(last - cum_buf[span, :]) * dt_buf[span, :])
        scaled = (conv_x[span, :].astype(f32) * end_weight).astype(bf16)
        new_state = lax.dot_general(
            conv_bc[span, pl.ds(0, state)], scaled, (((0,), (0,)), ((), ())),
            preferred_element_type=f32,
        )
        if block > 0:
            decay = spread_exact(jnp.broadcast_to(jnp.exp(last), (8, LANES)))[0:1]
            new_state = decay * states[block - 1] + new_state
        states[block] = new_state
        prefixes.append(prefix)
        prefix = prefix + last

    for j in range(devices):
        sum_out[j] = states[blocks - 1, pl.ds(j * share, share), :].astype(bf16)
    rate_out[...] = jnp.broadcast_to(prefix, (8, LANES))

    sum_copies, rate_copies = [], []
    for o in range(1, devices):
        sum_copies.append(
            remote(
                sum_out.at[seq_peer[o]], sum_in.at[o], sum_send.at[o], sum_recv.at[o],
                "seq", seq_peer[o],
            )
        )
        rate_copies.append(
            remote(
                rate_out, rate_in.at[o], rate_send.at[o], rate_recv.at[o], "seq", seq_peer[o]
            )
        )
    for a, b in zip(sum_copies, rate_copies):
        b.start()
        a.start()

    def gate_step(block, carry):
        fill_gate(block * SPAN, SPAN)
        return carry

    lax.fori_loop(0, blocks, gate_step, 0)

    row_index = lax.broadcasted_iota(jnp.int32, (LANES, LANES), 0)
    col_index = lax.broadcasted_iota(jnp.int32, (LANES, LANES), 1)
    causal = row_index >= col_index
    lane_index = lax.broadcasted_iota(jnp.int32, (SPAN, LANES), 1)
    pair = LANES // head_size

    def inside(block):
        span = pl.ds(pl.multiple_of(block * SPAN, SPAN), SPAN)
        running = cum_buf[span, :]
        running_t = running.T
        steps_t = dt_buf[span, :].T
        scores = lax.dot_general(
            conv_bc[span, pl.ds(state, state)], conv_bc[span, pl.ds(0, state)],
            (((1,), (1,)), ((), ())), preferred_element_type=f32,
        )
        half = SPAN // 2
        for strip in range(strips):
            lanes = pl.ds(strip * LANES, LANES)
            value = conv_x[span, lanes]
            upper, bottom, stacked_top, stacked = [], [], [], []
            for member in range(pair):
                head = strip * pair + member
                column = running[:, head : head + 1]
                line = running_t[head : head + 1, :]
                steps_line = steps_t[head : head + 1, :]

                def weights(r, c):
                    rs, cs = slice(r * half, (r + 1) * half), slice(c * half, (c + 1) * half)
                    gap = column[rs] - line[:, cs]
                    if r == c:
                        gap = jnp.where(causal, gap, -1e30)
                    return (scores[rs, cs] * jnp.exp(gap) * steps_line[:, cs]).astype(bf16)

                upper.append(weights(0, 0))
                bottom.extend([weights(1, 0), weights(1, 1)])
                mine = jnp.where(lane_index // head_size == member, value, jnp.zeros_like(value))
                stacked_top.append(mine[:half])
                stacked.append(mine)
            top_out = jnp.dot(
                jnp.concatenate(upper, axis=1), jnp.concatenate(stacked_top, axis=0),
                preferred_element_type=f32,
            )
            bottom_out = jnp.dot(
                jnp.concatenate(bottom, axis=1), jnp.concatenate(stacked, axis=0),
                preferred_element_type=f32,
            )
            both = jnp.concatenate([top_out, bottom_out], axis=0)
            y_buf[span, lanes] = both + skip_wide[:, strip * LANES : (strip + 1) * LANES] * value.astype(f32)

    def inside_step(block, carry):
        inside(block)
        return carry

    for a, b in zip(sum_copies, rate_copies):
        b.wait()
        a.wait()
    sum_in[0] = sum_out[me]
    rate_in[0] = rate_out[...]

    running_state = jnp.zeros((share, width), f32)
    for i in range(devices):
        slot = lax.rem(me - i + devices, devices)
        carry_out[slot] = running_state.astype(bf16)
        decay = spread_exact(jnp.exp(rate_in[slot]))[0:1]
        running_state = decay * running_state + sum_in[slot].astype(f32)

    carry_copies = []
    for o in range(1, devices):
        carry_copies.append(
            remote(
                carry_out.at[o], carry_in.at[o], carry_send.at[o], carry_recv.at[o],
                "seq", seq_back[o],
            )
        )
    for copy in carry_copies:
        copy.start()
    lax.fori_loop(0, blocks, inside_step, 0)
    load_proj.wait()
    for copy in carry_copies:
        copy.wait()
    carry_in[0] = carry_out[0]
    for j in range(devices):
        slot = lax.rem(j - me + devices, devices)
        carried[pl.ds(j * share, share), :] = carry_in[slot].astype(f32)

    for block in range(blocks):
        entry_decay = spread_exact(jnp.broadcast_to(jnp.exp(prefixes[block]), (8, LANES)))[0:1]
        entering = entry_decay * carried[...]
        if block > 0:
            entering = entering + states[block - 1]
        entered[block] = entering.astype(bf16)

    unit = chip_rows // 3 if chip_rows % 3 == 0 and SPAN % (chip_rows // 3) == 0 else 64

    def cross_unit(base):
        span = pl.ds(pl.multiple_of(base, 16), unit)
        block = base // SPAN
        growth = jnp.concatenate(in_two(jnp.exp(cum_buf[span, :])), axis=1)
        partial_sum = jnp.zeros((unit, LANES), f32)
        for column in range(0, width, tile):
            lanes = pl.ds(column, tile)
            cross = jnp.dot(
                conv_bc[span, pl.ds(state, state)], entered[block, :, lanes],
                preferred_element_type=f32,
            )
            scale = jnp.dot(
                growth, spread_two[:, column : column + tile], preferred_element_type=f32
            )
            gated = (y_buf[span, lanes] + scale * cross) * gate[span, lanes]
            squared = gated * gated
            for lower in range(0, tile, LANES):
                partial_sum = partial_sum + squared[:, lower : lower + LANES]
            normed[span, lanes] = (gated * norm_gain_ref[lanes].reshape(1, tile)).astype(bf16)
        inv_col[span, :] = partial_sum

    def cross_chip(o):
        base = lax.rem(chip + o, chips) * chip_rows

        def step(k, carry):
            cross_unit(base + k * unit)
            return carry

        lax.fori_loop(0, chip_rows // unit, step, 0)

    pieces = proj.shape[1] // PIECE
    jobs = [(o, q) for o in list(range(1, chips)) + [0] for q in range(pieces)]

    def pair_copy(o, q):
        return remote(
            pair_out.at[o, q], pair_in.at[o, q], pair_send.at[o, q], pair_recv.at[o, q],
            "head", partner,
        )

    def chip_copy(o, q):
        target = lax.rem(chip + o, chips) * CORES + core
        return remote(
            chip_out.at[o - 1, q], chip_in.at[o - 1, q], chip_send.at[o, q], chip_recv.at[o, q],
            "head", target,
        )

    def product(o, q, whose):
        base = lax.rem(chip + o, chips) * CORES * own_rows
        here = pl.ds(pl.multiple_of(base + whose * own_rows, 16), own_rows)
        return jnp.dot(normed[here, :], proj[:, pl.ds(q * PIECE, PIECE)], preferred_element_type=f32)

    def start_job(o, q):
        pair_out[o, q] = product(o, q, 1 - core).astype(bf16)
        pair_copy(o, q).start()

    def finish_job(o, q):
        result = product(o, q, core)
        pair_copy(o, q).wait()
        result = result + pair_in[o, q].astype(f32)
        if o > 0:
            chip_out[o - 1, q] = result.astype(bf16)
            chip_copy(o, q).start()
        else:
            keep[q] = result

    def send_squares():
        own_squares = jnp.concatenate(
            [
                jnp.sum(inv_col[pl.ds(block * SPAN, SPAN), :].T, axis=0, keepdims=True)
                for block in range(blocks)
            ],
            axis=1,
        )
        sq_out[...] = own_squares
        copies = [
            remote(sq_out, sq_in.at[o], sq_send.at[o], sq_recv.at[o], "head", head_peer[o])
            for o in range(1, groups)
        ]
        for copy in copies:
            copy.start()
        return own_squares, copies

    cross_chip(1)
    for index, job in enumerate(jobs):
        o, q = job
        if q == 0 and 1 < o:
            cross_chip(o)
        if q == 0 and o == 0:
            cross_chip(0)
            own_squares, sq_copies = send_squares()
        start_job(*job)
        if index > 0:
            finish_job(*jobs[index - 1])
    finish_job(*jobs[-1])

    for copy in sq_copies:
        copy.wait()
    total = own_squares
    for o in range(1, groups):
        total = total + sq_in[o]
    inverse = lax.rsqrt(total / total_width + norm_floor)
    for block in range(blocks):
        part = jnp.broadcast_to(inverse[:, block * SPAN : (block + 1) * SPAN], (LANES, SPAN)).T
        inv_col[pl.ds(block * SPAN, SPAN), :] = part
    own_inverse = inv_col[own, :]

    for q in range(pieces):
        result = keep[q]
        for o in range(1, chips):
            chip_copy(o, q).wait()
            result = result + chip_in[o - 1, q].astype(f32)
        for lower in range(0, PIECE, LANES):
            out_ref[:, pl.ds(q * PIECE + lower, LANES)] = (
                result[:, lower : lower + LANES] * own_inverse
            ).astype(bf16)

    for feed in range(feeds):
        mate_copy(0, feed).wait_send()
        for o in range(1, chips):
            row_copy(o, feed).wait_send()
            mate_copy(o, feed).wait_send()


def layer_call(*operands):
    tokens, _, inner_proj, outer_proj, kernel_x, kernel_bc, _, _, dt_bias, _, _, _, out_proj = operands
    devices, groups = lax.axis_size("seq"), lax.axis_size("head")
    own_rows, model = tokens.shape
    width, taps, state = kernel_x.shape[1], kernel_x.shape[0], kernel_bc.shape[1] // 2
    rows = own_rows * groups
    blocks, share = rows // SPAN, state // devices
    chips, strips, feeds = groups // CORES, width // LANES, model // FEED
    chip_rows = own_rows * CORES
    pieces = model // PIECE
    sizes = (devices, groups, rows, model, width, state, taps, dt_bias.shape[0])
    f32, bf16 = jnp.float32, jnp.bfloat16
    sem = pltpu.SemaphoreType.DMA
    vmem, hbm = pl.BlockSpec(memory_space=pltpu.VMEM), pl.BlockSpec(memory_space=pl.ANY)
    return pl.pallas_call(
        functools.partial(layer_kernel, sizes),
        out_shape=jax.ShapeDtypeStruct((own_rows, model), bf16),
        in_specs=[hbm, vmem, hbm, hbm] + [vmem] * 8 + [hbm],
        out_specs=vmem,
        scratch_shapes=[
            pltpu.VMEM((rows, model), bf16),
            pltpu.VMEM((own_rows, model), bf16),
            pltpu.VMEM((2, strips, DEPTH, 2, LANES), bf16),
            pltpu.VMEM((model, width), bf16),
            pltpu.VMEM((model, width), bf16),
            pltpu.VMEM(outer_proj.shape, bf16),
            pltpu.VMEM(out_proj.shape, bf16),
            pltpu.VMEM((rows, width), f32),
            pltpu.VMEM((rows + 8, width), f32),
            pltpu.VMEM((rows + 8, 2 * state), f32),
            pltpu.VMEM((rows, LANES), f32),
            pltpu.VMEM((HALO, width), f32),
            pltpu.VMEM((HALO, 2 * state), f32),
            pltpu.VMEM((HALO, width), f32),
            pltpu.VMEM((HALO, 2 * state), f32),
            pltpu.VMEM((rows, width), bf16),
            pltpu.VMEM((rows, 2 * state), bf16),
            pltpu.VMEM((rows, width), f32),
            pltpu.VMEM((rows, LANES), f32),
            pltpu.VMEM((blocks, state, width), f32),
            pltpu.VMEM((state, width), f32),
            pltpu.VMEM((devices, share, width), bf16),
            pltpu.VMEM((devices, share, width), bf16),
            pltpu.VMEM((8, LANES), f32),
            pltpu.VMEM((devices, 8, LANES), f32),
            pltpu.VMEM((devices, share, width), bf16),
            pltpu.VMEM((devices, share, width), bf16),
            pltpu.VMEM((rows, width), bf16),
            pltpu.VMEM((1, rows), f32),
            pltpu.VMEM((groups, 1, rows), f32),
            pltpu.VMEM((rows, LANES), f32),
            pltpu.VMEM((blocks, state, width), bf16),
            pltpu.VMEM((chips, pieces, own_rows, PIECE), bf16),
            pltpu.VMEM((chips, pieces, own_rows, PIECE), bf16),
            pltpu.VMEM((chips - 1, pieces, own_rows, PIECE), bf16),
            pltpu.VMEM((chips - 1, pieces, own_rows, PIECE), bf16),
            pltpu.VMEM((pieces, own_rows, PIECE), f32),
            pltpu.VMEM((8, LANES), f32),
            sem,
            sem((2, strips)),
            sem((2,)),
            sem((chips, feeds)),
            sem((chips, feeds)),
            sem((chips, feeds)),
            sem((chips, feeds)),
            sem((4,)),
            sem((devices,)),
            sem((devices,)),
            sem((devices,)),
            sem((devices,)),
            sem((devices,)),
            sem((devices,)),
            sem((groups,)),
            sem((groups,)),
            sem((chips, pieces)),
            sem((chips, pieces)),
            sem((chips, pieces)),
            sem((chips, pieces)),
        ],
        compiler_params=pltpu.CompilerParams(
            collective_id=0, has_side_effects=True, vmem_limit_bytes=67043328
        ),
    )(*operands)


def on_device(*args):
    operands = list(args)
    operands[3] = operands[3].T
    return layer_call(*operands)


def solution(mesh):
    return jax.shard_map(
        on_device,
        mesh=mesh,
        in_specs=(
            P(("seq", "head"), None),
            P(),
            P(None, None, "head"),
            P(),
            P(None, "head"),
            P(),
            P("head"),
            P(),
            P("head"),
            P("head"),
            P("head"),
            P("head"),
            P("head", None),
        ),
        out_specs=P(("seq", "head"), None),
        check_vma=False,
    )
```

```python
import functools

import jax
import jax.numpy as jnp
from jax import lax
from jax.experimental import pallas as pl
from jax.experimental.pallas import tpu as pltpu
from jax.sharding import PartitionSpec as P

SPAN = 256
HALO = 8
LANES = 128
PIECE = 256
CORES = 2
FEED = 256
DEPTH = 256
SLOTS = 4

norm_floor = 0.1


def silu(value):
    half = 0.5 * value
    return half * jnp.tanh(half) + half


def softplus(value):
    small = jnp.exp(-jnp.abs(value))
    series = small * (1.0 - small * (0.5 - small * (1.0 / 3.0 - small * 0.25)))
    return jnp.maximum(value, 0.0) + jnp.where(small < 0.03, series, jnp.log(1.0 + small))


def in_two(value):
    top = value.astype(jnp.bfloat16)
    return top, (value - top.astype(jnp.float32)).astype(jnp.bfloat16)


def in_three(value):
    top = value.astype(jnp.bfloat16)
    rest = value - top.astype(jnp.float32)
    middle = rest.astype(jnp.bfloat16)
    return top, middle, (rest - middle.astype(jnp.float32)).astype(jnp.bfloat16)


def layer_kernel(
    sizes,
    tokens_hbm,
    pre_gain_ref,
    inner_hbm,
    outer_hbm,
    kernel_x_ref,
    kernel_bc_ref,
    offset_x_ref,
    offset_bc_ref,
    dt_bias_ref,
    a_log_ref,
    skip_gain_ref,
    norm_gain_ref,
    proj_hbm,
    out_ref,
    tok,
    tok_in,
    raw,
    gate_w,
    inner_w,
    outer_w,
    proj,
    gate,
    ext_x,
    ext_bc,
    dt_buf,
    halo_x,
    halo_bc,
    halo_x_out,
    halo_bc_out,
    conv_x,
    conv_bc,
    y_buf,
    cum_buf,
    states,
    carried,
    sum_out,
    sum_in,
    rate_out,
    rate_in,
    carry_out,
    carry_in,
    normed,
    sq_out,
    sq_in,
    inv_col,
    entered,
    pair_out,
    pair_in,
    chip_out,
    chip_in,
    keep,
    small,
    tok_sem,
    raw_sems,
    load_sems,
    row_send,
    row_recv,
    mate_send,
    mate_recv,
    halo_sems,
    sum_send,
    sum_recv,
    rate_send,
    rate_recv,
    carry_send,
    carry_recv,
    sq_send,
    sq_recv,
    pair_send,
    pair_recv,
    chip_send,
    chip_recv,
):
    devices, groups, rows, model, width, state, taps, head_count = sizes
    f32, bf16 = jnp.float32, jnp.bfloat16
    head_size = width // head_count
    blocks = rows // SPAN
    share = state // devices
    total_width = width * groups
    own_rows = rows // groups
    chips = groups // CORES
    chip_rows = own_rows * CORES
    feeds = model // FEED
    steps = model // DEPTH
    strips = width // LANES
    me = lax.axis_index("seq")
    group = lax.axis_index("head")
    chip, core = group // CORES, lax.rem(group, CORES)
    partner = group + 1 - 2 * core
    seq_peer = [lax.rem(me + o, devices) for o in range(devices)]
    seq_back = [lax.rem(me - o + devices, devices) for o in range(devices)]
    head_peer = [lax.rem(group + o, groups) for o in range(groups)]

    def remote(src, dst, send, recv, axis, peer):
        return pltpu.make_async_remote_copy(
            src_ref=src, dst_ref=dst, send_sem=send, recv_sem=recv, device_id={axis: peer}
        )

    own = pl.ds(pl.multiple_of(group * own_rows, 16), own_rows)
    load_tok = pltpu.make_async_copy(tokens_hbm, tok_in, tok_sem)
    load_tok.start()

    def raw_copy(step, slot, strip):
        return pltpu.make_async_copy(
            inner_hbm.at[pl.ds(pl.multiple_of(step * DEPTH, DEPTH), DEPTH), :, pl.ds(strip * LANES, LANES)],
            raw.at[slot, strip],
            raw_sems.at[slot, strip],
        )

    for strip in range(strips):
        raw_copy(0, 0, strip).start()
    load_outer = pltpu.make_async_copy(outer_hbm, outer_w, load_sems.at[0])
    load_outer.start()
    for slot in range(1, SLOTS):
        for strip in range(strips):
            raw_copy(slot, slot, strip).start()
    load_proj = pltpu.make_async_copy(proj_hbm, proj, load_sems.at[1])

    barrier = pltpu.get_barrier_semaphore()
    for o in range(1, devices):
        pl.semaphore_signal(barrier, 1, device_id={"seq": seq_peer[o]})
    for o in range(1, groups):
        pl.semaphore_signal(barrier, 1, device_id={"head": head_peer[o]})

    small[...] = jnp.zeros_like(small)
    small[0:1, 0:head_count] = dt_bias_ref[...].reshape(1, head_count)
    small[1:2, 0:head_count] = -jnp.exp(a_log_ref[...].reshape(1, head_count))
    small[2:3, 0:head_count] = skip_gain_ref[...].reshape(1, head_count)

    def clear(k, carry):
        row = pl.multiple_of(k * 64, 64)
        ext_x[pl.ds(8 + row, 64), :] = jnp.zeros((64, width), f32)
        ext_bc[pl.ds(8 + row, 64), :] = jnp.zeros((64, 2 * state), f32)
        dt_buf[pl.ds(row, 64), :] = jnp.zeros((64, LANES), f32)
        return carry

    group_rows = 48 if own_rows % 48 == 0 else 16

    def normalise(k, carry):
        row = pl.multiple_of(k * group_rows, 16)
        here = pl.ds(row, group_rows)
        squares = jnp.zeros((group_rows, LANES), f32)
        for column in range(0, model, LANES):
            value = tok_in[here, pl.ds(column, LANES)].astype(f32)
            squares = squares + value * value
        inverse = lax.rsqrt(jnp.sum(squares, axis=1, keepdims=True) / model + norm_floor)
        there = pl.ds(pl.multiple_of(group * own_rows + row, 16), group_rows)
        for column in range(0, model, LANES):
            lanes = pl.ds(column, LANES)
            value = tok_in[here, lanes].astype(f32)
            tok[there, lanes] = (
                value * inverse * pre_gain_ref[lanes].reshape(1, LANES)
            ).astype(bf16)
        return carry

    load_tok.wait()
    lax.fori_loop(0, own_rows // group_rows, normalise, 0)
    pl.semaphore_wait(barrier, devices + groups - 2)

    def feed_at(chip_index, core_index, feed):
        begin = pl.multiple_of((chip_index * CORES + core_index) * own_rows, 16)
        return tok.at[pl.ds(begin, own_rows), pl.ds(pl.multiple_of(feed * FEED, FEED), FEED)]

    def mate_copy(o, feed):
        piece = feed_at(lax.rem(chip - o + chips, chips), core, feed)
        return remote(piece, piece, mate_send.at[o, feed], mate_recv.at[o, feed], "head", partner)

    def row_copy(o, feed):
        piece = feed_at(chip, core, feed)
        target = lax.rem(chip + o, chips) * CORES + core
        return remote(piece, piece, row_send.at[o, feed], row_recv.at[o, feed], "head", target)

    for feed in range(feeds):
        for o in range(1, chips):
            row_copy(o, feed).start()
    for feed in range(feeds):
        mate_copy(0, feed).start()
    lax.fori_loop(0, rows // 64, clear, 0)

    out_row = lax.broadcasted_iota(jnp.int32, (DEPTH, DEPTH), 0)
    in_row = lax.broadcasted_iota(jnp.int32, (DEPTH, DEPTH), 1)
    half_depth = DEPTH // 2
    parting = (
        in_row == jnp.where(out_row < half_depth, 2 * out_row, 2 * (out_row - half_depth) + 1)
    ).astype(f32).astype(bf16)

    def separate(step, slot):
        for lower in range(0, strips, 2):
            members = range(lower, min(lower + 2, strips))
            columns = pl.ds(lower * LANES, len(members) * LANES)
            for part in range(2):
                parts = [
                    raw.at[slot, m].reshape(2 * DEPTH, LANES)[pl.ds(part * DEPTH, DEPTH), :]
                    for m in members
                ]
                both = jnp.dot(
                    parting, jnp.concatenate(parts, axis=1), preferred_element_type=f32
                ).astype(bf16)
                begin = pl.multiple_of(step * DEPTH + part * half_depth, half_depth)
                gate_w[pl.ds(begin, half_depth), columns] = both[:half_depth]
                inner_w[pl.ds(begin, half_depth), columns] = both[half_depth:]

    tile = 256 if width % 256 == 0 else LANES

    def rows_of(base, begin, depth):
        return tok[pl.ds(pl.multiple_of(base, 16), chip_rows), pl.ds(begin, depth)]

    def gather_into(target, offset, base, weight, begin, depth):
        here = pl.ds(pl.multiple_of(base + offset, 8), chip_rows)
        for column in range(0, width, tile):
            columns = pl.ds(column, tile)
            target[here, columns] += jnp.dot(
                rows_of(base, begin, depth), weight[pl.ds(begin, depth), columns],
                preferred_element_type=f32,
            )

    def gather_outer(base, begin, depth):
        result = lax.dot_general(
            rows_of(base, begin, depth), outer_w[:, pl.ds(begin, depth)], (((1,), (1,)), ((), ())),
            preferred_element_type=f32,
        )
        ext_bc[pl.ds(pl.multiple_of(base + 8, 8), chip_rows), :] += result[:, : 2 * state]
        raw_columns = result.shape[1] - 2 * state
        dt_buf[pl.ds(pl.multiple_of(base, 8), chip_rows), pl.ds(0, raw_columns)] += result[:, 2 * state :]

    local_base = pl.multiple_of(chip * chip_rows, 32)
    load_outer.wait()

    def wait_raw(step, slot):
        for strip in range(strips):
            raw_copy(step, slot, strip).wait()

    def local_product(step):
        begin = pl.multiple_of(step * DEPTH, DEPTH)
        gather_into(ext_x, 8, local_base, inner_w, begin, DEPTH)
        gather_outer(local_base, begin, DEPTH)

    def local_step(step, carry):
        slot = lax.rem(step, SLOTS)
        wait_raw(step, slot)
        mate_copy(0, step - 1).wait_recv()
        local_product(step - 1)
        separate(step, slot)

        @pl.when(step + SLOTS < steps)
        def _():
            for strip in range(strips):
                raw_copy(step + SLOTS, slot, strip).start()

        return carry

    wait_raw(0, 0)
    separate(0, 0)
    for strip in range(strips):
        raw_copy(SLOTS, 0, strip).start()
    lax.fori_loop(1, steps, local_step, 0)
    mate_copy(0, steps - 1).wait_recv()
    local_product(steps - 1)
    load_proj.start()

    bias_row, rate_row = small[0:1, :], small[1:2, :]
    own_lane = lax.broadcasted_iota(jnp.int32, (32, LANES), 1) < head_count

    def finish_rows(base):
        def step(k, carry):
            row = pl.multiple_of(base + k * 32, 32)
            here, lower = pl.ds(row, 32), pl.ds(row + 8, 32)
            for target, columns in ((ext_x, width), (ext_bc, 2 * state)):
                for column in range(0, columns, LANES):
                    lanes = pl.ds(column, LANES)
                    target[lower, lanes] = target[lower, lanes].astype(bf16).astype(f32)
            raw_steps = pltpu.roll(dt_buf[here, :], lax.rem(LANES - group * head_count, LANES), 1)
            dt_buf[here, :] = jnp.where(own_lane, softplus(raw_steps + bias_row), 0.0)
            return carry

        lax.fori_loop(0, chip_rows // 32, step, 0)

    def fill_gate(base, size):
        here = pl.ds(pl.multiple_of(base, 16), size)
        for column in range(0, width, tile):
            columns = pl.ds(column, tile)
            gate_in = jnp.dot(tok[here, :], gate_w[:, columns], preferred_element_type=f32)
            gate[here, columns] = silu(gate_in.astype(bf16).astype(f32))

    def convolve(source, weight, bias, target, columns, row):
        for lower in range(0, columns, LANES):
            lanes = pl.ds(lower, LANES)
            window = source[pl.ds(row, 40), lanes]
            total = jnp.broadcast_to(bias[lanes].reshape(1, LANES), (32, LANES))
            for tap in range(taps):
                shift = 8 - taps + 1 + tap
                total = total + weight[tap : tap + 1, lanes] * window[shift : shift + 32]
            target[pl.ds(row, 32), lanes] = silu(total).astype(bf16)

    def convolve_rows(begin, first, last):
        def step(k, carry):
            row = pl.multiple_of(begin + k * 32, 32)
            convolve(ext_bc, kernel_bc_ref, offset_bc_ref, conv_bc, 2 * state, row)
            convolve(ext_x, kernel_x_ref, offset_x_ref, conv_x, width, row)
            return carry

        lax.fori_loop(first, last, step, 0)

    finish_rows(local_base)
    convolve_rows(local_base, 1, chip_rows // 32)

    def far_base(o):
        return pl.multiple_of(lax.rem(chip - o + chips, chips) * chip_rows, 32)

    def take_feed(o, feed):
        row_copy(o, feed).wait_recv()
        mate_copy(o, feed).start()

    def far_step(o, feed):
        mate_copy(o, feed).wait_recv()
        begin = pl.multiple_of(feed * FEED, FEED)
        gather_into(ext_x, 8, far_base(o), inner_w, begin, FEED)
        gather_outer(far_base(o), begin, FEED)

    for o in range(1, chips):
        take_feed(o, 0)

        def far_loop(feed, carry):
            take_feed(o, feed + 1)
            far_step(o, feed)
            return carry

        lax.fori_loop(0, feeds - 1, far_loop, 0)
        far_step(o, feeds - 1)
        finish_rows(far_base(o))

    halo_x_out[...] = ext_x[pl.ds(rows, HALO), :]
    halo_bc_out[...] = ext_bc[pl.ds(rows, HALO), :]
    halo_copies = [
        remote(halo_x_out, halo_x, halo_sems.at[0], halo_sems.at[1], "seq", seq_peer[1]),
        remote(halo_bc_out, halo_bc, halo_sems.at[2], halo_sems.at[3], "seq", seq_peer[1]),
    ]
    for copy in halo_copies:
        copy.start()
    for o in range(1, chips):
        convolve_rows(far_base(o), 1, chip_rows // 32)
    for block in range(1, chips):
        convolve_rows(block * chip_rows, 0, 1)

    head_of_lane = lax.broadcasted_iota(jnp.int32, (LANES, width), 1) // head_size
    spread = (
        (head_of_lane == lax.broadcasted_iota(jnp.int32, (LANES, width), 0)).astype(f32).astype(bf16)
    )
    spread_two = jnp.concatenate([spread, spread], axis=0)
    lower_tri = (
        lax.broadcasted_iota(jnp.int32, (SPAN, SPAN), 0)
        >= lax.broadcasted_iota(jnp.int32, (SPAN, SPAN), 1)
    ).astype(f32).astype(bf16)

    def spread_rows(value):
        return jnp.dot(
            jnp.concatenate(in_two(value), axis=1), spread_two, preferred_element_type=f32
        )

    def spread_exact(value):
        total = 0.0
        for part in in_three(value):
            total = total + jnp.dot(part, spread, preferred_element_type=f32)
        return total

    skip_wide = spread_exact(jnp.broadcast_to(small[2:3, :], (8, LANES)))[0:1]
    lasts = []
    for block in range(blocks):
        span = pl.ds(block * SPAN, SPAN)
        parts = jnp.dot(
            lower_tri, jnp.concatenate(in_three(dt_buf[span, :] * rate_row), axis=1),
            preferred_element_type=f32,
        )
        running = parts[:, :LANES] + parts[:, LANES : 2 * LANES] + parts[:, 2 * LANES :]
        cum_buf[span, :] = running
        lasts.append(running[SPAN - 1 : SPAN, :])

    for copy in halo_copies:
        copy.wait()
    first = me > 0
    ext_x[0:8, :] = jnp.where(first, halo_x[...], 0.0)
    ext_bc[0:8, :] = jnp.where(first, halo_bc[...], 0.0)
    convolve_rows(0, 0, 1)

    prefix = jnp.zeros((1, LANES), f32)
    prefixes = []
    for block in range(blocks):
        span = pl.ds(block * SPAN, SPAN)
        last = lasts[block]
        end_weight = spread_rows(jnp.exp(last - cum_buf[span, :]) * dt_buf[span, :])
        scaled = (conv_x[span, :].astype(f32) * end_weight).astype(bf16)
        new_state = lax.dot_general(
            conv_bc[span, pl.ds(0, state)], scaled, (((0,), (0,)), ((), ())),
            preferred_element_type=f32,
        )
        if block > 0:
            decay = spread_exact(jnp.broadcast_to(jnp.exp(last), (8, LANES)))[0:1]
            new_state = decay * states[block - 1] + new_state
        states[block] = new_state
        prefixes.append(prefix)
        prefix = prefix + last

    for j in range(devices):
        sum_out[j] = states[blocks - 1, pl.ds(j * share, share), :].astype(bf16)
    rate_out[...] = jnp.broadcast_to(prefix, (8, LANES))

    sum_copies, rate_copies = [], []
    for o in range(1, devices):
        sum_copies.append(
            remote(
                sum_out.at[seq_peer[o]], sum_in.at[o], sum_send.at[o], sum_recv.at[o],
                "seq", seq_peer[o],
            )
        )
        rate_copies.append(
            remote(
                rate_out, rate_in.at[o], rate_send.at[o], rate_recv.at[o], "seq", seq_peer[o]
            )
        )
    for a, b in zip(sum_copies, rate_copies):
        b.start()
        a.start()

    def gate_step(block, carry):
        fill_gate(block * SPAN, SPAN)
        return carry

    lax.fori_loop(0, blocks, gate_step, 0)

    row_index = lax.broadcasted_iota(jnp.int32, (LANES, LANES), 0)
    col_index = lax.broadcasted_iota(jnp.int32, (LANES, LANES), 1)
    causal = row_index >= col_index
    lane_index = lax.broadcasted_iota(jnp.int32, (SPAN, LANES), 1)
    pair = LANES // head_size

    def inside(block):
        span = pl.ds(pl.multiple_of(block * SPAN, SPAN), SPAN)
        running = cum_buf[span, :]
        running_t = running.T
        steps_t = dt_buf[span, :].T
        scores = lax.dot_general(
            conv_bc[span, pl.ds(state, state)], conv_bc[span, pl.ds(0, state)],
            (((1,), (1,)), ((), ())), preferred_element_type=f32,
        )
        half = SPAN // 2
        for strip in range(strips):
            lanes = pl.ds(strip * LANES, LANES)
            value = conv_x[span, lanes]
            upper, bottom, stacked_top, stacked = [], [], [], []
            for member in range(pair):
                head = strip * pair + member
                column = running[:, head : head + 1]
                line = running_t[head : head + 1, :]
                steps_line = steps_t[head : head + 1, :]

                def weights(r, c):
                    rs, cs = slice(r * half, (r + 1) * half), slice(c * half, (c + 1) * half)
                    gap = column[rs] - line[:, cs]
                    if r == c:
                        gap = jnp.where(causal, gap, -1e30)
                    return (scores[rs, cs] * jnp.exp(gap) * steps_line[:, cs]).astype(bf16)

                upper.append(weights(0, 0))
                bottom.extend([weights(1, 0), weights(1, 1)])
                mine = jnp.where(lane_index // head_size == member, value, jnp.zeros_like(value))
                stacked_top.append(mine[:half])
                stacked.append(mine)
            top_out = jnp.dot(
                jnp.concatenate(upper, axis=1), jnp.concatenate(stacked_top, axis=0),
                preferred_element_type=f32,
            )
            bottom_out = jnp.dot(
                jnp.concatenate(bottom, axis=1), jnp.concatenate(stacked, axis=0),
                preferred_element_type=f32,
            )
            both = jnp.concatenate([top_out, bottom_out], axis=0)
            y_buf[span, lanes] = both + skip_wide[:, strip * LANES : (strip + 1) * LANES] * value.astype(f32)

    def inside_step(block, carry):
        inside(block)
        return carry

    for a, b in zip(sum_copies, rate_copies):
        b.wait()
        a.wait()
    sum_in[0] = sum_out[me]
    rate_in[0] = rate_out[...]

    running_state = jnp.zeros((share, width), f32)
    for i in range(devices):
        slot = lax.rem(me - i + devices, devices)
        carry_out[slot] = running_state.astype(bf16)
        decay = spread_exact(jnp.exp(rate_in[slot]))[0:1]
        running_state = decay * running_state + sum_in[slot].astype(f32)

    carry_copies = []
    for o in range(1, devices):
        carry_copies.append(
            remote(
                carry_out.at[o], carry_in.at[o], carry_send.at[o], carry_recv.at[o],
                "seq", seq_back[o],
            )
        )
    for copy in carry_copies:
        copy.start()
    lax.fori_loop(0, blocks, inside_step, 0)
    load_proj.wait()
    for copy in carry_copies:
        copy.wait()
    carry_in[0] = carry_out[0]
    for j in range(devices):
        slot = lax.rem(j - me + devices, devices)
        carried[pl.ds(j * share, share), :] = carry_in[slot].astype(f32)

    for block in range(blocks):
        entry_decay = spread_exact(jnp.broadcast_to(jnp.exp(prefixes[block]), (8, LANES)))[0:1]
        entering = entry_decay * carried[...]
        if block > 0:
            entering = entering + states[block - 1]
        entered[block] = entering.astype(bf16)

    unit = chip_rows // 3 if chip_rows % 3 == 0 and SPAN % (chip_rows // 3) == 0 else 64

    def cross_unit(base):
        span = pl.ds(pl.multiple_of(base, 16), unit)
        block = base // SPAN
        growth = jnp.concatenate(in_two(jnp.exp(cum_buf[span, :])), axis=1)
        partial_sum = jnp.zeros((unit, LANES), f32)
        for column in range(0, width, tile):
            lanes = pl.ds(column, tile)
            cross = jnp.dot(
                conv_bc[span, pl.ds(state, state)], entered[block, :, lanes],
                preferred_element_type=f32,
            )
            scale = jnp.dot(
                growth, spread_two[:, column : column + tile], preferred_element_type=f32
            )
            gated = (y_buf[span, lanes] + scale * cross) * gate[span, lanes]
            squared = gated * gated
            for lower in range(0, tile, LANES):
                partial_sum = partial_sum + squared[:, lower : lower + LANES]
            normed[span, lanes] = (gated * norm_gain_ref[lanes].reshape(1, tile)).astype(bf16)
        inv_col[span, :] = partial_sum

    def cross_chip(o):
        base = lax.rem(chip + o, chips) * chip_rows

        def step(k, carry):
            cross_unit(base + k * unit)
            return carry

        lax.fori_loop(0, chip_rows // unit, step, 0)

    pieces = proj.shape[1] // PIECE
    jobs = [(o, q) for o in list(range(1, chips)) + [0] for q in range(pieces)]

    def pair_copy(o, q):
        return remote(
            pair_out.at[o, q], pair_in.at[o, q], pair_send.at[o, q], pair_recv.at[o, q],
            "head", partner,
        )

    def chip_copy(o, q):
        target = lax.rem(chip + o, chips) * CORES + core
        return remote(
            chip_out.at[o - 1, q], chip_in.at[o - 1, q], chip_send.at[o, q], chip_recv.at[o, q],
            "head", target,
        )

    def product(o, q, whose):
        base = lax.rem(chip + o, chips) * CORES * own_rows
        here = pl.ds(pl.multiple_of(base + whose * own_rows, 16), own_rows)
        return jnp.dot(normed[here, :], proj[:, pl.ds(q * PIECE, PIECE)], preferred_element_type=f32)

    def start_job(o, q):
        pair_out[o, q] = product(o, q, 1 - core).astype(bf16)
        pair_copy(o, q).start()

    def finish_job(o, q):
        result = product(o, q, core)
        pair_copy(o, q).wait()
        result = result + pair_in[o, q].astype(f32)
        if o > 0:
            chip_out[o - 1, q] = result.astype(bf16)
            chip_copy(o, q).start()
        else:
            keep[q] = result

    def send_squares():
        own_squares = jnp.concatenate(
            [
                jnp.sum(inv_col[pl.ds(block * SPAN, SPAN), :].T, axis=0, keepdims=True)
                for block in range(blocks)
            ],
            axis=1,
        )
        sq_out[...] = own_squares
        copies = [
            remote(sq_out, sq_in.at[o], sq_send.at[o], sq_recv.at[o], "head", head_peer[o])
            for o in range(1, groups)
        ]
        for copy in copies:
            copy.start()
        return own_squares, copies

    cross_chip(1)
    for index, job in enumerate(jobs):
        o, q = job
        if q == 0 and 1 < o:
            cross_chip(o)
        if q == 0 and o == 0:
            cross_chip(0)
            own_squares, sq_copies = send_squares()
        start_job(*job)
        if index > 0:
            finish_job(*jobs[index - 1])
    finish_job(*jobs[-1])

    for copy in sq_copies:
        copy.wait()
    total = own_squares
    for o in range(1, groups):
        total = total + sq_in[o]
    inverse = lax.rsqrt(total / total_width + norm_floor)
    for block in range(blocks):
        part = jnp.broadcast_to(inverse[:, block * SPAN : (block + 1) * SPAN], (LANES, SPAN)).T
        inv_col[pl.ds(block * SPAN, SPAN), :] = part
    own_inverse = inv_col[own, :]

    for q in range(pieces):
        result = keep[q]
        for o in range(1, chips):
            chip_copy(o, q).wait()
            result = result + chip_in[o - 1, q].astype(f32)
        for lower in range(0, PIECE, LANES):
            out_ref[:, pl.ds(q * PIECE + lower, LANES)] = (
                result[:, lower : lower + LANES] * own_inverse
            ).astype(bf16)

    for feed in range(feeds):
        mate_copy(0, feed).wait_send()
        for o in range(1, chips):
            row_copy(o, feed).wait_send()
            mate_copy(o, feed).wait_send()


def layer_call(*operands):
    tokens, _, inner_proj, outer_proj, kernel_x, kernel_bc, _, _, dt_bias, _, _, _, out_proj = operands
    devices, groups = lax.axis_size("seq"), lax.axis_size("head")
    own_rows, model = tokens.shape
    width, taps, state = kernel_x.shape[1], kernel_x.shape[0], kernel_bc.shape[1] // 2
    rows = own_rows * groups
    blocks, share = rows // SPAN, state // devices
    chips, strips, feeds = groups // CORES, width // LANES, model // FEED
    chip_rows = own_rows * CORES
    pieces = model // PIECE
    sizes = (devices, groups, rows, model, width, state, taps, dt_bias.shape[0])
    f32, bf16 = jnp.float32, jnp.bfloat16
    sem = pltpu.SemaphoreType.DMA
    vmem, hbm = pl.BlockSpec(memory_space=pltpu.VMEM), pl.BlockSpec(memory_space=pl.ANY)
    return pl.pallas_call(
        functools.partial(layer_kernel, sizes),
        out_shape=jax.ShapeDtypeStruct((own_rows, model), bf16),
        in_specs=[hbm, vmem, hbm, hbm] + [vmem] * 8 + [hbm],
        out_specs=vmem,
        scratch_shapes=[
            pltpu.VMEM((rows, model), bf16),
            pltpu.VMEM((own_rows, model), bf16),
            pltpu.VMEM((SLOTS, strips, DEPTH, 2, LANES), bf16),
            pltpu.VMEM((model, width), bf16),
            pltpu.VMEM((model, width), bf16),
            pltpu.VMEM(outer_proj.shape, bf16),
            pltpu.VMEM(out_proj.shape, bf16),
            pltpu.VMEM((rows, width), f32),
            pltpu.VMEM((rows + 8, width), f32),
            pltpu.VMEM((rows + 8, 2 * state), f32),
            pltpu.VMEM((rows, LANES), f32),
            pltpu.VMEM((HALO, width), f32),
            pltpu.VMEM((HALO, 2 * state), f32),
            pltpu.VMEM((HALO, width), f32),
            pltpu.VMEM((HALO, 2 * state), f32),
            pltpu.VMEM((rows, width), bf16),
            pltpu.VMEM((rows, 2 * state), bf16),
            pltpu.VMEM((rows, width), f32),
            pltpu.VMEM((rows, LANES), f32),
            pltpu.VMEM((blocks, state, width), f32),
            pltpu.VMEM((state, width), f32),
            pltpu.VMEM((devices, share, width), bf16),
            pltpu.VMEM((devices, share, width), bf16),
            pltpu.VMEM((8, LANES), f32),
            pltpu.VMEM((devices, 8, LANES), f32),
            pltpu.VMEM((devices, share, width), bf16),
            pltpu.VMEM((devices, share, width), bf16),
            pltpu.VMEM((rows, width), bf16),
            pltpu.VMEM((1, rows), f32),
            pltpu.VMEM((groups, 1, rows), f32),
            pltpu.VMEM((rows, LANES), f32),
            pltpu.VMEM((blocks, state, width), bf16),
            pltpu.VMEM((chips, pieces, own_rows, PIECE), bf16),
            pltpu.VMEM((chips, pieces, own_rows, PIECE), bf16),
            pltpu.VMEM((chips - 1, pieces, own_rows, PIECE), bf16),
            pltpu.VMEM((chips - 1, pieces, own_rows, PIECE), bf16),
            pltpu.VMEM((pieces, own_rows, PIECE), f32),
            pltpu.VMEM((8, LANES), f32),
            sem,
            sem((SLOTS, strips)),
            sem((2,)),
            sem((chips, feeds)),
            sem((chips, feeds)),
            sem((chips, feeds)),
            sem((chips, feeds)),
            sem((4,)),
            sem((devices,)),
            sem((devices,)),
            sem((devices,)),
            sem((devices,)),
            sem((devices,)),
            sem((devices,)),
            sem((groups,)),
            sem((groups,)),
            sem((chips, pieces)),
            sem((chips, pieces)),
            sem((chips, pieces)),
            sem((chips, pieces)),
        ],
        compiler_params=pltpu.CompilerParams(
            collective_id=0, has_side_effects=True, vmem_limit_bytes=67043328
        ),
    )(*operands)


def on_device(*args):
    operands = list(args)
    operands[3] = operands[3].T
    return layer_call(*operands)


def solution(mesh):
    return jax.shard_map(
        on_device,
        mesh=mesh,
        in_specs=(
            P(("seq", "head"), None),
            P(),
            P(None, None, "head"),
            P(),
            P(None, "head"),
            P(),
            P("head"),
            P(),
            P("head"),
            P("head"),
            P("head"),
            P("head"),
            P("head", None),
        ),
        out_specs=P(("seq", "head"), None),
        check_vma=False,
    )
```
